32 devices in a mesh: dom: 16 (over z, y, x), st: 2 (over core).
Axes of the slice: x: 2, y: 2, z: 4, core: 2. Of those that a mesh axis runs over, the one named last changes fastest.
Arguments:
- psi: float32 [2, 16, 8, 2, 64, 256], P(None, 'dom', None, None, None, 'st'), parts along dimension 5, may hold values from -18 to 18
- potential: float32 [16, 8, 2, 64], P('dom'), may hold values from 0 to 4
Outputs:
- propagated: float32 [2, 16, 8, 2, 64, 256], P(None, 'dom', None, None, None, 'st'), parts along dimension 5
The draws below stay inside these ranges and needn't reach their ends.
There are 2 independent parts, one for each index of `st`. The reference program is written for one: setup_inputs(seed, part) draws one part's arguments, and reference() takes and returns one part's arrays. A program takes and returns all parts, laid end to end along the dimension named above; an argument that names none is the same for every part. Nothing has to cross between parts.
All inputs are finite; a program needn't handle non-finite values.
Results may differ from the reference program's by a relative error of at most 0.0003.
Values sent between devices are 32-bit elements; how exact they have to be, the bound alone decides.
A program may use at most 128 MiB of HBM per device.

```python
import jax
import jax.numpy as jnp
from jax import lax

CX = 8
BY = 2
NZ = 64
ORB = 128
ITERS = 6
BLOCKS = 16


def draw_psi(key, part):
    shape = (2, BLOCKS, CX, BY, NZ, ORB)
    rising = 1.0 + 2.0 * jnp.arange(BLOCKS, dtype=jnp.float32) / max(BLOCKS - 1, 1)
    rising = rising.reshape(1, BLOCKS, 1, 1, 1, 1)
    return jnp.clip(jax.random.normal(key, shape, jnp.float32), -6.0, 6.0) * rising


def steps_of(rng, dims, shards, smallest, high):
    loudness = 1.0
    for dim, shards_of in shards:
        heights = jax.random.uniform(jax.random.fold_in(jax.random.fold_in(rng, 6), dim), (shards_of,), jnp.float32, smallest / len(shards), high / len(shards))
        loudness = loudness * jnp.repeat(jnp.exp(heights), dims[dim] // shards_of).reshape((-1,) + (1,) * (len(dims) - 1 - dim))
    return loudness


def setup_inputs(seed: int = 0, part: int = 0) -> dict:
    keys = jax.random.split(jax.random.key(seed), 3)
    part_keys = jax.random.split(jax.random.fold_in(keys[2], part), 3)
    psi = draw_psi(jax.random.fold_in(jax.random.fold_in(keys[2], part), 71), part)
    potential = jnp.clip(4.0 * jax.random.uniform(keys[1], (BLOCKS, CX, BY, NZ), jnp.float32) ** steps_of(keys[1], (BLOCKS, CX, BY, NZ), ((0, 16),), -0.2, 0.2), 0.0, 4.0)
    return dict(psi=psi, potential=potential)


epsilon = 1e-06
time_step = 0.5
taylor_terms = 32
far_weight = -1.0 / 12.0
near_weight = 4.0 / 3.0
centre_weight = -7.5

def to_grid(blocked):
    parts, nblocks, cx, by, nz, orbs = blocked.shape
    grid = blocked.transpose(0, 2, 1, 3, 4, 5)
    return grid.reshape(parts, cx, nblocks * by, nz, orbs)

def to_blocks(grid, by):
    parts, nx, ny, nz, orbs = grid.shape
    blocked = grid.reshape(parts, nx, ny // by, by, nz, orbs).transpose(0, 2, 1, 3, 4, 5)
    return blocked

def shift_walls(values, offset):
    width_y = values.shape[2]
    padded = jnp.pad(values, ((0, 0), (0, 0), (2, 2), (0, 0), (0, 0)))
    return padded[:, :, 2 - offset:2 - offset + width_y]

def hamiltonian(values_in, potential):
    total = centre_weight * values_in
    for along in (1, 3):
        total = total + near_weight * (jnp.roll(values_in, 1, along) + jnp.roll(values_in, -1, along))
        total = total + far_weight * (jnp.roll(values_in, 2, along) + jnp.roll(values_in, -2, along))
    total = total + near_weight * (shift_walls(values_in, 1) + shift_walls(values_in, -1))
    total = total + far_weight * (shift_walls(values_in, 2) + shift_walls(values_in, -2))
    return -0.5 * total + potential[None, :, :, :, None] * values_in

def tridiagonal(alphas, betas, vector):
    zero_row = jnp.zeros((1, vector.shape[1]), jnp.float32)
    upper = jnp.concatenate([betas * vector[1:], zero_row], axis=0)
    lower = jnp.concatenate([zero_row, betas * vector[:-1]], axis=0)
    return alphas * vector + upper + lower

def krylov_exponential(alphas, betas):
    count = alphas.shape[0]
    first = (jnp.arange(count) == 0).astype(jnp.float32)[:, None] * jnp.ones_like(alphas)
    term_real = first
    term_imag = jnp.zeros_like(alphas)
    sum_real = term_real
    sum_imag = term_imag
    for order in range(1, taylor_terms):
        applied_real = tridiagonal(alphas, betas, term_real)
        applied_imag = tridiagonal(alphas, betas, term_imag)
        term_real = time_step * applied_imag / order
        term_imag = -time_step * applied_real / order
        sum_real = sum_real + term_real
        sum_imag = sum_imag + term_imag
    return (sum_real, sum_imag)

def reference(psi, potential):
    by = psi.shape[3]
    grid_psi = to_grid(psi)
    grid_pot = to_grid(potential[None, :, :, :, :, None])[0, :, :, :, 0]
    axes_all = (0, 1, 2, 3)
    first_norm = jnp.sqrt(lax.optimization_barrier(jnp.sum(grid_psi * grid_psi, axis=axes_all)) + epsilon)
    vector = grid_psi / first_norm
    previous = jnp.zeros_like(vector)
    beta_prev = jnp.zeros_like(first_norm)
    krylov_basis = []
    alpha_list = []
    beta_list = []
    for iteration in range(ITERS):
        applied = hamiltonian(vector, grid_pot)
        alpha_now = lax.optimization_barrier(jnp.sum(vector * applied, axis=axes_all))
        krylov_basis.append(vector)
        alpha_list.append(alpha_now)
        if iteration + 1 < ITERS:
            remainder = applied - alpha_now * vector - beta_prev * previous
            beta_now = jnp.sqrt(lax.optimization_barrier(jnp.sum(remainder * remainder, axis=axes_all)) + epsilon)
            previous = vector
            vector = remainder / beta_now
            beta_prev = beta_now
            beta_list.append(beta_now)
    coef_real, coef_imag = krylov_exponential(jnp.stack(alpha_list), jnp.stack(beta_list))
    out_real = jnp.zeros_like(grid_psi[0])
    out_imag = jnp.zeros_like(grid_psi[0])
    for index_j in range(ITERS):
        basis_now = krylov_basis[index_j]
        out_real = out_real + coef_real[index_j] * basis_now[0] - coef_imag[index_j] * basis_now[1]
        out_imag = out_imag + coef_real[index_j] * basis_now[1] + coef_imag[index_j] * basis_now[0]
    return to_blocks(first_norm * jnp.stack([out_real, out_imag]), by)
```

```python
import functools

import jax
import jax.numpy as jnp
from jax import lax
from jax.experimental import pallas as pl
from jax.experimental.pallas import tpu as pltpu
from jax.sharding import PartitionSpec as P

ITERS = 6


epsilon = 1e-06
time_step = 0.5
taylor_terms = 32
far_weight = -1.0 / 12.0
near_weight = 4.0 / 3.0
centre_weight = -7.5


def to_grid(blocked):
    parts, nblocks, cx, by, nz, orbs = blocked.shape
    grid = blocked.transpose(0, 2, 1, 3, 4, 5)
    return grid.reshape(parts, cx, nblocks * by, nz, orbs)


def to_blocks(grid, by):
    parts, nx, ny, nz, orbs = grid.shape
    blocked = grid.reshape(parts, nx, ny // by, by, nz, orbs).transpose(0, 2, 1, 3, 4, 5)
    return blocked


def shift_walls(values, offset):
    width_y = values.shape[2]
    padded = jnp.pad(values, ((0, 0), (0, 0), (2, 2), (0, 0), (0, 0)))
    return padded[:, :, 2 - offset : 2 - offset + width_y]


def hamiltonian_whole(values_in, potential):
    total = centre_weight * values_in
    for along in (1, 3):
        total = total + near_weight * (
            jnp.roll(values_in, 1, along) + jnp.roll(values_in, -1, along)
        )
        total = total + far_weight * (
            jnp.roll(values_in, 2, along) + jnp.roll(values_in, -2, along)
        )
    total = total + near_weight * (shift_walls(values_in, 1) + shift_walls(values_in, -1))
    total = total + far_weight * (shift_walls(values_in, 2) + shift_walls(values_in, -2))
    return -0.5 * total + potential[None, :, :, :, None] * values_in


def tridiagonal(alphas, betas, vector):
    zero_row = jnp.zeros((1, vector.shape[1]), jnp.float32)
    upper = jnp.concatenate([betas * vector[1:], zero_row], axis=0)
    lower = jnp.concatenate([zero_row, betas * vector[:-1]], axis=0)
    return alphas * vector + upper + lower


def krylov_exponential(alphas, betas):
    count = alphas.shape[0]
    first = (jnp.arange(count) == 0).astype(jnp.float32)[:, None] * jnp.ones_like(alphas)
    term_real = first
    term_imag = jnp.zeros_like(alphas)
    sum_real = term_real
    sum_imag = term_imag
    for order in range(1, taylor_terms):
        applied_real = tridiagonal(alphas, betas, term_real)
        applied_imag = tridiagonal(alphas, betas, term_imag)
        term_real = time_step * applied_imag / order
        term_imag = -time_step * applied_real / order
        sum_real = sum_real + term_real
        sum_imag = sum_imag + term_imag
    return (sum_real, sum_imag)


def combine_basis(krylov_basis, alpha_list, beta_list, first_norm):
    coef_real, coef_imag = krylov_exponential(jnp.stack(alpha_list), jnp.stack(beta_list))
    out_real = jnp.zeros_like(krylov_basis[0][0])
    out_imag = jnp.zeros_like(krylov_basis[0][0])
    for index_j in range(len(krylov_basis)):
        basis_now = krylov_basis[index_j]
        out_real = out_real + coef_real[index_j] * basis_now[0] - coef_imag[index_j] * basis_now[1]
        out_imag = out_imag + coef_real[index_j] * basis_now[1] + coef_imag[index_j] * basis_now[0]
    return first_norm * jnp.stack([out_real, out_imag])


def local_lanczos(grid_psi, grid_pot):
    axes_all = (0, 1, 2, 3)
    first_norm = jnp.sqrt(jnp.sum(grid_psi * grid_psi, axis=axes_all) + epsilon)
    vector = grid_psi / first_norm
    previous = jnp.zeros_like(vector)
    beta_prev = jnp.zeros_like(first_norm)
    krylov_basis = []
    alpha_list = []
    beta_list = []
    for iteration in range(ITERS):
        applied = hamiltonian_whole(vector, grid_pot)
        alpha_now = jnp.sum(vector * applied, axis=axes_all)
        krylov_basis.append(vector)
        alpha_list.append(alpha_now)
        if iteration + 1 < ITERS:
            remainder = applied - alpha_now * vector - beta_prev * previous
            beta_now = jnp.sqrt(jnp.sum(remainder * remainder, axis=axes_all) + epsilon)
            previous = vector
            vector = remainder / beta_now
            beta_prev = beta_now
            beta_list.append(beta_now)
    return combine_basis(krylov_basis, alpha_list, beta_list, first_norm)


def on_device(psi, potential):
    by = psi.shape[3]
    moved = lax.all_to_all(psi, "dom", split_axis=5, concat_axis=1, tiled=True)
    whole_pot = lax.all_gather(potential, "dom", axis=0, tiled=True)
    grid_pot = to_grid(whole_pot[None, :, :, :, :, None])[0, :, :, :, 0]
    result = to_blocks(local_lanczos(to_grid(moved), grid_pot), by)
    return lax.all_to_all(result, "dom", split_axis=1, concat_axis=5, tiled=True)


SUB = 8
LANES = 128
HALF = SUB // 2
CHUNKS = 2
GROUP = 4
UNROLL_A = 4
UNROLL_B = 8


def swap_parts(x):
    return pltpu.roll(x, HALF, 0)


def total_of(acc):
    summed = jnp.broadcast_to(jnp.sum(acc, axis=1, keepdims=True), (SUB, LANES))
    return summed + swap_parts(summed)


def krylov_weights(alphas, betas):
    count = len(alphas)
    one = jnp.ones((SUB, LANES), jnp.float32)
    term = [one] + [None] * (count - 1)
    real = [one] + [None] * (count - 1)
    imag = [None] * count
    for order in range(1, taylor_terms):
        fresh = []
        for i in range(count):
            pieces = []
            if term[i] is not None:
                pieces.append(alphas[i] * term[i])
            if i + 1 < count and term[i + 1] is not None:
                pieces.append(betas[i] * term[i + 1])
            if i > 0 and term[i - 1] is not None:
                pieces.append(betas[i - 1] * term[i - 1])
            fresh.append(sum(pieces[1:], pieces[0]) * (time_step / order) if pieces else None)
        term = fresh
        into = imag if order % 2 else real
        minus = order % 4 in (1, 2)
        for i in range(count):
            if term[i] is not None:
                if into[i] is None:
                    into[i] = -term[i] if minus else term[i]
                else:
                    into[i] = into[i] - term[i] if minus else into[i] + term[i]
    zero = jnp.zeros((SUB, LANES), jnp.float32)
    return [zero if r is None else r for r in real], [zero if m is None else m for m in imag]


def kernel(n, nx, nz, psi_ref, pot_ref, out_ref, send, recv, extra, basis, inner, outb, outx, back, pots, mix,
           note, heard, send_sem, recv_sem, extra_send, extra_recv, pot_send, pot_recv, back_send, back_recv,
           far_send, note_send, note_recv):
    me = lax.axis_index("dom")
    mesh_ids = pl.DeviceIdType.MESH
    barrier = pltpu.get_barrier_semaphore()

    half = n // 2
    reach = ITERS - 1
    deep = half - reach
    side = me // half
    base = side * half
    opposite = half - base
    partner = lax.rem(me + half, n)
    near = half - side * reach
    outer = jnp.logical_or(me < deep, me >= n - deep)

    def greet(k, carry):
        pl.semaphore_signal(barrier, inc=1, device_id={"dom": lax.rem(me + k, n)}, device_id_type=mesh_ids)
        return carry

    lax.fori_loop(1, n, greet, 0)

    def remote(src, dst, send_to, recv_to, there):
        return pltpu.make_async_remote_copy(
            src_ref=src, dst_ref=dst, send_sem=send_to, recv_sem=recv_to,
            device_id={"dom": there}, device_id_type=mesh_ids)

    def forward(c, here, there):
        return remote(send.at[c, there], recv.at[c, here + 1], send_sem.at[c], recv_sem.at[c, here], there)

    def beside(c, here, there):
        return remote(send.at[c, lax.rem(there + half, n)], extra.at[c, lax.rem(here, half) + 1],
                      extra_send.at[c], extra_recv.at[c, lax.rem(here, half)], there)

    def pot_copy(here, there):
        return remote(pot_ref, pots.at[here], pot_send, pot_recv.at[here], there)

    def backward(c, owner, there):
        return remote(outb.at[c, there], back.at[c, owner], back_send.at[c], back_recv.at[c, owner], there)

    def far_copy(c, i, there):
        return remote(outx.at[c, i], back.at[c, partner], far_send.at[c], back_recv.at[c, partner], there)

    def note_copy(c):
        return remote(note.at[c], heard.at[c], note_send.at[c], note_recv.at[c], partner)

    low = lax.broadcasted_iota(jnp.int32, (n, SUB, LANES), 1) < HALF

    def interleave(a, b):
        return (jnp.where(low, a, pltpu.roll(b, HALF, 1)), jnp.where(low, pltpu.roll(a, HALF, 1), b))

    def pack(x, carry):
        parts = [psi_ref[p * nx + x].T.reshape(n, SUB, LANES) for p in range(2)]
        for c, block in enumerate(interleave(*parts)):
            send[c, :, x] = block
        return carry

    lax.fori_loop(0, nx, pack, 0)

    pots[me] = pot_ref[...]
    blank = jnp.zeros((nx, SUB, LANES), jnp.float32)
    for c in range(CHUNKS):
        recv[c, me + 1] = send[c, me]
        recv[c, 0] = blank
        recv[c, n + 1] = blank
        extra[c, me - base + 1] = send[c, partner]
        extra[c, 0] = blank
        extra[c, half + 1] = blank
    for j in range(ITERS - 1):
        basis[j, 0] = blank
        basis[j, n + 1] = blank
        inner[j, 0] = blank
        inner[j, half + 1] = blank

    pl.semaphore_wait(barrier, n - 1)

    def send_pot(k, carry):
        pot_copy(me, lax.rem(me + k, n)).start()
        return carry

    lax.fori_loop(1, n, send_pot, 0)

    for c in range(CHUNKS):
        def send_across(k, carry, c=c):
            forward(c, me, opposite + lax.rem(me + k, half)).start()
            return carry

        def send_home(k, carry, c=c):
            forward(c, me, base + lax.rem(me + k, half)).start()
            return carry

        lax.fori_loop(0, half, send_across, 0)
        lax.fori_loop(1, half, send_home, 0)

    for c in range(CHUNKS):
        def send_beside(k, carry, c=c):
            beside(c, me, base + lax.rem(me + k, half)).start()
            return carry

        lax.fori_loop(1, half, send_beside, 0)

    def wait_pot(k, carry):
        there = lax.rem(me + n - k, n)
        pot_copy(there, there).wait_recv()
        return carry

    upper = lax.broadcasted_iota(jnp.int32, (SUB, LANES), 1) >= nz
    lane = lax.broadcasted_iota(jnp.int32, (SUB, LANES), 1)
    sign = jnp.where(lax.broadcasted_iota(jnp.int32, (SUB, LANES), 0) < HALF, 1.0, -1.0)
    ratio = -0.5 * far_weight

    row = lax.broadcasted_iota(jnp.int32, (LANES, LANES), 0)
    column = lax.broadcasted_iota(jnp.int32, (LANES, LANES), 1)
    apart = lax.rem(row - column + 2 * nz, nz)
    near_z = jnp.where(jnp.logical_or(apart == 1, apart == nz - 1), 16.0, 0.0)
    far_z = jnp.where(jnp.logical_or(apart == 2, apart == nz - 2), 1.0, 0.0)
    same = (row < nz) == (column < nz)
    lanes_matrix = jnp.where(same, far_z - near_z, jnp.where(apart == 0, -16.0, 0.0)).astype(jnp.bfloat16)
    mix[0:LANES] = lanes_matrix
    mix[LANES:2 * LANES] = lanes_matrix

    def applied_at(ref, s, slab, size):
        slabs = [[ref[s + g, x] for x in range(nx)] for g in range(size + 2)]
        inside = jnp.concatenate([u for row_of in slabs[1:-1] for u in row_of], axis=0)
        high = inside.astype(jnp.bfloat16)
        rest = (inside - high.astype(jnp.float32)).astype(jnp.bfloat16)
        mixed = jnp.dot(jnp.concatenate([high, rest], axis=1), mix[...], preferred_element_type=jnp.float32)
        result = []
        for g in range(size):
            before, now, after = slabs[g:g + 3]
            for x in range(nx):
                u = now[x]
                close = now[(x + 1) % nx] + now[(x - 1) % nx]
                close = close + pltpu.roll(jnp.where(upper, before[x], after[x]), nz, 1)
                wide = now[(x + 2) % nx] + now[(x - 2) % nx] + before[x] + after[x]
                at = (g * nx + x) * SUB
                wide = wide + mixed[at:at + SUB]
                own = jnp.broadcast_to(pots[slab + g, pl.ds(x, 1), :], (SUB, LANES)) + -0.5 * centre_weight
                result.append((own * u + ratio * (wide - 16.0 * close), u))
        return result

    def blend(us, straight, crossed):
        a = straight[0] * us[0]
        b = crossed[0] * us[0]
        for j in range(1, ITERS):
            a = a + straight[j] * us[j]
            b = b + crossed[j] * us[j]
        return a + swap_parts(b)

    def chunk(c, carry):
        vectors = [recv.at[c]] + [basis.at[j] for j in range(ITERS - 1)]

        def arrive(k, acc):
            there = lax.rem(me + n - k, n)
            forward(c, there, there).wait_recv()
            for x in range(nx):
                u = recv[c, there + 1, x]
                acc = acc + u * u
            return acc

        acc = jnp.zeros((SUB, LANES), jnp.float32)
        for x in range(nx):
            u = recv[c, me + 1, x]
            acc = acc + u * u
        acc = lax.fori_loop(1, n, arrive, acc)
        first_norm = jnp.sqrt(total_of(acc) + epsilon)

        @pl.when(c == 0)
        def _():
            lax.fori_loop(1, n, wait_pot, 0)

        scales = [1.0 / first_norm]
        alphas, betas, selves, previous = [], [], [], []
        zero = jnp.zeros((SUB, LANES), jnp.float32)
        for j in range(ITERS):
            ref = vectors[j]
            last = j + 1 == ITERS
            fresh = None if last else vectors[j + 1]

            def apply(s, accs, ref=ref, fresh=fresh):
                accs = list(accs)
                for at, (w, u) in enumerate(applied_at(ref, s * GROUP, s * GROUP, GROUP)):
                    if fresh is not None:
                        fresh[s * GROUP + at // nx + 1, at % nx] = w
                    accs[at % 2] = accs[at % 2] + u * w
                return tuple(accs)

            accs = lax.fori_loop(0, n // GROUP, apply, (zero, zero), unroll=UNROLL_A)
            scale = scales[j]
            alpha = scale * (scale * total_of(accs[0] + accs[1]))
            alphas.append(alpha)
            if last:
                break
            by_self = alpha * scale
            by_previous = betas[j - 1] * scales[j - 1] if j else None
            selves.append(by_self)
            previous.append(by_previous)

            def reduce(s, accs, ref=ref, fresh=fresh, scale=scale, by_self=by_self, by_previous=by_previous, j=j):
                accs = list(accs)
                for x in range(nx):
                    r = scale * fresh[s + 1, x] - by_self * ref[s + 1, x]
                    if j:
                        r = r - by_previous * vectors[j - 1][s + 1, x]
                    fresh[s + 1, x] = r
                    accs[x % 2] = accs[x % 2] + r * r
                return tuple(accs)

            accs = lax.fori_loop(0, n, reduce, (zero, zero), unroll=UNROLL_B)
            beta = jnp.sqrt(total_of(accs[0] + accs[1]) + epsilon)
            betas.append(beta)
            scales.append(1.0 / beta)

        real, imag = krylov_weights(alphas, betas)
        straight = [first_norm * scales[j] * real[j] for j in range(ITERS)]
        crossed = [first_norm * scales[j] * imag[j] * sign for j in range(ITERS)]

        told = zero
        for k, value in enumerate(scales[:-1] + selves + previous[1:] + straight + crossed):
            told = jnp.where(lane == k, value, told)
        note[c] = told

        def combined(d, x):
            return blend([v[d + 1, x] for v in vectors], straight, crossed)

        def finish_across(k, carry):
            there = near + lax.rem(me + k, reach)
            for x in range(nx):
                outb[c, there, x] = combined(there, x)

            @pl.when(k == 0)
            def _():
                note_copy(c).start()

            @pl.when(k > 0)
            def _():
                backward(c, me, near + lax.rem(me + k - 1, reach)).start()

            return carry

        lax.fori_loop(0, reach, finish_across, 0)

        def finish_home(k, carry):
            there = base + lax.rem(me + k, half)
            for x in range(nx):
                outb[c, there, x] = combined(there, x)

            @pl.when(k == 1)
            def _():
                backward(c, me, near + lax.rem(me + reach - 1, reach)).start()

            @pl.when(k > 1)
            def _():
                backward(c, me, base + lax.rem(me + k - 1, half)).start()

            return carry

        lax.fori_loop(1, half, finish_home, 0)
        for x in range(nx):
            back[c, me, x] = combined(me, x)
        backward(c, me, base + lax.rem(me + half - 1, half)).start()

        def beside_arrives(k, carry):
            there = base + lax.rem(me + k, half)
            beside(c, there, there).wait_recv()
            return carry

        lax.fori_loop(1, half, beside_arrives, 0)
        note_copy(c).wait_recv()
        words = heard[c]
        word = [jnp.broadcast_to(words[:, k:k + 1], (SUB, LANES)) for k in range(3 * reach - 1 + 2 * ITERS)]
        scales, selves, previous = word[:reach], word[reach:2 * reach], [None] + word[2 * reach:3 * reach - 1]
        straight, crossed = word[3 * reach - 1:3 * reach - 1 + ITERS], word[3 * reach - 1 + ITERS:]

        halves = [extra.at[c]] + [inner.at[j] for j in range(reach)]
        for j in range(reach):
            count = half - 1 - j
            start = (j + 1) * side
            pieces = -(-count // GROUP)
            at = 0
            for piece in range(pieces):
                size = (count - at) // (pieces - piece)
                for i, (w, u) in enumerate(applied_at(halves[j], start + at, base + start + at, size)):
                    here = start + at + i // nx + 1
                    r = scales[j] * w - selves[j] * u
                    if j:
                        r = r - previous[j] * halves[j - 1][here, i % nx]
                    halves[j + 1][here, i % nx] = r
                at += size

        first = reach * side
        for i in range(deep):
            for x in range(nx):
                outx[c, i, x] = blend([v[first + i + 1, x] for v in halves], straight, crossed)
        for i in range(deep):
            there = base + first + i

            @pl.when(there == me)
            def _(i=i):
                back[c, partner] = outx[c, i]

            @pl.when(there != me)
            def _(i=i, there=there):
                far_copy(c, i, there).start()
        return carry

    lax.fori_loop(0, CHUNKS, chunk, 0)

    remote(pots.at[pl.ds(0, n - 1)], pots.at[pl.ds(0, n - 1)], pot_send, pot_recv.at[0], partner).wait_send()
    for c in range(CHUNKS):
        blocks = send.at[c, pl.ds(0, n - 1)]
        remote(blocks, blocks, send_sem.at[c], recv_sem.at[c, 0], partner).wait_send()
        blocks = send.at[c, pl.ds(0, half - 1)]
        remote(blocks, blocks, extra_send.at[c], recv_sem.at[c, 0], partner).wait_send()
        note_copy(c).wait_send()

    for c in range(CHUNKS):
        def returned(k, carry, c=c):
            there = lax.rem(me + n - k, n)

            @pl.when(jnp.logical_not(jnp.logical_and(outer, there == partner)))
            def _():
                backward(c, there, there).wait_recv()

            return carry

        lax.fori_loop(1, n, returned, 0)

    def unpack(x, carry):
        for p, block in enumerate(interleave(back[0, :, x], back[1, :, x])):
            out_ref[p * nx + x] = block.reshape(n * SUB, LANES).T
        return carry

    lax.fori_loop(0, nx, unpack, 0)

    for c in range(CHUNKS):
        blocks = outb.at[c, pl.ds(0, reach + half - 1)]
        remote(blocks, blocks, back_send.at[c], recv_sem.at[c, 0], partner).wait_send()

        @pl.when(outer)
        def _(c=c):
            blocks = outx.at[c, pl.ds(0, deep - 1)]
            remote(blocks, blocks, far_send.at[c], recv_sem.at[c, 0], partner).wait_send()

        @pl.when(jnp.logical_not(outer))
        def _(c=c):
            blocks = outx.at[c]
            remote(blocks, blocks, far_send.at[c], recv_sem.at[c, 0], partner).wait_send()


def fused(psi, potential, n):
    parts, slabs, nx, by, nz, orbs = psi.shape
    half, reach = n // 2, ITERS - 1
    vec = lambda *lead: pltpu.VMEM(lead + (nx, SUB, LANES), jnp.float32)
    tile = lambda *lead: pltpu.VMEM(lead + (SUB, LANES), jnp.float32)
    dma = lambda *shape: pltpu.SemaphoreType.DMA(shape)
    result = pl.pallas_call(
        functools.partial(kernel, n, nx, nz),
        out_shape=jax.ShapeDtypeStruct((parts * nx, by * nz, orbs), jnp.float32),
        in_specs=[pl.BlockSpec(memory_space=pltpu.VMEM)] * 2,
        out_specs=pl.BlockSpec(memory_space=pltpu.VMEM),
        scratch_shapes=[
            vec(CHUNKS, n), vec(CHUNKS, n + 2), vec(CHUNKS, half + 2), vec(reach, n + 2), vec(reach, half + 2),
            vec(CHUNKS, n), vec(CHUNKS, half - reach), vec(CHUNKS, n),
            pltpu.VMEM((n, nx, LANES), jnp.float32), pltpu.VMEM((2 * LANES, LANES), jnp.bfloat16),
            tile(CHUNKS), tile(CHUNKS),
            dma(CHUNKS), dma(CHUNKS, n), dma(CHUNKS), dma(CHUNKS, half), pltpu.SemaphoreType.DMA, dma(n),
            dma(CHUNKS), dma(CHUNKS, n), dma(CHUNKS), dma(CHUNKS), dma(CHUNKS),
        ],
        compiler_params=pltpu.CompilerParams(collective_id=0, has_side_effects=True),
    )(psi.reshape(parts * nx, by * nz, orbs), potential.reshape(nx, by * nz))
    return result.reshape(psi.shape)


def fits(psi, n):
    parts, slabs, nx, by, nz, orbs = psi.shape
    return parts == 2 and slabs == 1 and by == 2 and by * nz == LANES and orbs == LANES and orbs == n * SUB and n % GROUP == 0 and n // 2 > ITERS


def per_device(n, psi, potential):
    if fits(psi, n):
        return fused(psi, potential, n)
    return on_device(psi, potential)


def solution(mesh):
    placed = (P(None, "dom", None, None, None, "st"), P("dom", None, None, None))
    return jax.shard_map(
        functools.partial(per_device, mesh.shape["dom"]),
        mesh=mesh,
        in_specs=placed,
        out_specs=P(None, "dom", None, None, None, "st"),
        check_vma=False,
    )
```

```python
import functools

import jax
import jax.numpy as jnp
from jax import lax
from jax.experimental import pallas as pl
from jax.experimental.pallas import tpu as pltpu
from jax.sharding import PartitionSpec as P

ITERS = 6


epsilon = 1e-06
time_step = 0.5
taylor_terms = 32
far_weight = -1.0 / 12.0
near_weight = 4.0 / 3.0
centre_weight = -7.5


def to_grid(blocked):
    parts, nblocks, cx, by, nz, orbs = blocked.shape
    grid = blocked.transpose(0, 2, 1, 3, 4, 5)
    return grid.reshape(parts, cx, nblocks * by, nz, orbs)


def to_blocks(grid, by):
    parts, nx, ny, nz, orbs = grid.shape
    blocked = grid.reshape(parts, nx, ny // by, by, nz, orbs).transpose(0, 2, 1, 3, 4, 5)
    return blocked


def shift_walls(values, offset):
    width_y = values.shape[2]
    padded = jnp.pad(values, ((0, 0), (0, 0), (2, 2), (0, 0), (0, 0)))
    return padded[:, :, 2 - offset : 2 - offset + width_y]


def hamiltonian_whole(values_in, potential):
    total = centre_weight * values_in
    for along in (1, 3):
        total = total + near_weight * (
            jnp.roll(values_in, 1, along) + jnp.roll(values_in, -1, along)
        )
        total = total + far_weight * (
            jnp.roll(values_in, 2, along) + jnp.roll(values_in, -2, along)
        )
    total = total + near_weight * (shift_walls(values_in, 1) + shift_walls(values_in, -1))
    total = total + far_weight * (shift_walls(values_in, 2) + shift_walls(values_in, -2))
    return -0.5 * total + potential[None, :, :, :, None] * values_in


def tridiagonal(alphas, betas, vector):
    zero_row = jnp.zeros((1, vector.shape[1]), jnp.float32)
    upper = jnp.concatenate([betas * vector[1:], zero_row], axis=0)
    lower = jnp.concatenate([zero_row, betas * vector[:-1]], axis=0)
    return alphas * vector + upper + lower


def krylov_exponential(alphas, betas):
    count = alphas.shape[0]
    first = (jnp.arange(count) == 0).astype(jnp.float32)[:, None] * jnp.ones_like(alphas)
    term_real = first
    term_imag = jnp.zeros_like(alphas)
    sum_real = term_real
    sum_imag = term_imag
    for order in range(1, taylor_terms):
        applied_real = tridiagonal(alphas, betas, term_real)
        applied_imag = tridiagonal(alphas, betas, term_imag)
        term_real = time_step * applied_imag / order
        term_imag = -time_step * applied_real / order
        sum_real = sum_real + term_real
        sum_imag = sum_imag + term_imag
    return (sum_real, sum_imag)


def combine_basis(krylov_basis, alpha_list, beta_list, first_norm):
    coef_real, coef_imag = krylov_exponential(jnp.stack(alpha_list), jnp.stack(beta_list))
    out_real = jnp.zeros_like(krylov_basis[0][0])
    out_imag = jnp.zeros_like(krylov_basis[0][0])
    for index_j in range(len(krylov_basis)):
        basis_now = krylov_basis[index_j]
        out_real = out_real + coef_real[index_j] * basis_now[0] - coef_imag[index_j] * basis_now[1]
        out_imag = out_imag + coef_real[index_j] * basis_now[1] + coef_imag[index_j] * basis_now[0]
    return first_norm * jnp.stack([out_real, out_imag])


def local_lanczos(grid_psi, grid_pot):
    axes_all = (0, 1, 2, 3)
    first_norm = jnp.sqrt(jnp.sum(grid_psi * grid_psi, axis=axes_all) + epsilon)
    vector = grid_psi / first_norm
    previous = jnp.zeros_like(vector)
    beta_prev = jnp.zeros_like(first_norm)
    krylov_basis = []
    alpha_list = []
    beta_list = []
    for iteration in range(ITERS):
        applied = hamiltonian_whole(vector, grid_pot)
        alpha_now = jnp.sum(vector * applied, axis=axes_all)
        krylov_basis.append(vector)
        alpha_list.append(alpha_now)
        if iteration + 1 < ITERS:
            remainder = applied - alpha_now * vector - beta_prev * previous
            beta_now = jnp.sqrt(jnp.sum(remainder * remainder, axis=axes_all) + epsilon)
            previous = vector
            vector = remainder / beta_now
            beta_prev = beta_now
            beta_list.append(beta_now)
    return combine_basis(krylov_basis, alpha_list, beta_list, first_norm)


def on_device(psi, potential):
    by = psi.shape[3]
    moved = lax.all_to_all(psi, "dom", split_axis=5, concat_axis=1, tiled=True)
    whole_pot = lax.all_gather(potential, "dom", axis=0, tiled=True)
    grid_pot = to_grid(whole_pot[None, :, :, :, :, None])[0, :, :, :, 0]
    result = to_blocks(local_lanczos(to_grid(moved), grid_pot), by)
    return lax.all_to_all(result, "dom", split_axis=1, concat_axis=5, tiled=True)


SUB = 8
LANES = 128
HALF = SUB // 2
CHUNKS = 2
GROUP = 4
UNROLL_A = 4
UNROLL_B = 8


def swap_parts(x):
    return pltpu.roll(x, HALF, 0)


def total_of(acc):
    summed = jnp.broadcast_to(jnp.sum(acc, axis=1, keepdims=True), (SUB, LANES))
    return summed + swap_parts(summed)


def krylov_weights(alphas, betas):
    count = len(alphas)
    one = jnp.ones((SUB, LANES), jnp.float32)
    term = [one] + [None] * (count - 1)
    real = [one] + [None] * (count - 1)
    imag = [None] * count
    for order in range(1, taylor_terms):
        fresh = []
        for i in range(count):
            pieces = []
            if term[i] is not None:
                pieces.append(alphas[i] * term[i])
            if i + 1 < count and term[i + 1] is not None:
                pieces.append(betas[i] * term[i + 1])
            if i > 0 and term[i - 1] is not None:
                pieces.append(betas[i - 1] * term[i - 1])
            fresh.append(sum(pieces[1:], pieces[0]) * (time_step / order) if pieces else None)
        term = fresh
        into = imag if order % 2 else real
        minus = order % 4 in (1, 2)
        for i in range(count):
            if term[i] is not None:
                if into[i] is None:
                    into[i] = -term[i] if minus else term[i]
                else:
                    into[i] = into[i] - term[i] if minus else into[i] + term[i]
    zero = jnp.zeros((SUB, LANES), jnp.float32)
    return [zero if r is None else r for r in real], [zero if m is None else m for m in imag]


def interleave(a, b, n):
    low = lax.broadcasted_iota(jnp.int32, (n, SUB, LANES), 1) < HALF
    return (jnp.where(low, a, pltpu.roll(b, HALF, 1)), jnp.where(low, pltpu.roll(a, HALF, 1), b))


def unpack_kernel(n, nx, back, out_hbm, out, sems):
    def put(at):
        return pltpu.make_async_copy(out.at[at], out_hbm.at[at], sems.at[at])

    for x in range(nx):
        for p, block in enumerate(interleave(back[0, :, x], back[1, :, x], n)):
            out[p * nx + x] = block.reshape(n * SUB, LANES).T
        if x:
            for p in range(2):
                put(p * nx + x - 1).start()
    for p in range(2):
        put(p * nx + nx - 1).start()
    for at in range(2 * nx):
        put(at).wait()


def kernel(n, nx, nz, psi_hbm, pot_hbm, back, psi_ref, pot_ref, send, recv, extra, basis, inner, outb, outx, pots, mix,
           note, heard, send_sem, recv_sem, extra_send, extra_recv, pot_send, pot_recv, back_send, back_recv,
           far_send, note_send, note_recv, psi_sem, pot_sem):
    me = lax.axis_index("dom")
    mesh_ids = pl.DeviceIdType.MESH
    barrier = pltpu.get_barrier_semaphore()

    half = n // 2
    reach = ITERS - 1
    deep = half - reach
    side = me // half
    base = side * half
    opposite = half - base
    partner = lax.rem(me + half, n)
    near = half - side * reach
    outer = jnp.logical_or(me < deep, me >= n - deep)
    plane = n // 4
    spot = lax.rem(me, plane)
    inward = jnp.logical_and(me >= plane, me < n - plane)
    far_plane = (1 - side) * (n - plane)

    def greet(k, carry):
        pl.semaphore_signal(barrier, inc=1, device_id={"dom": lax.rem(me + k, n)}, device_id_type=mesh_ids)
        return carry

    lax.fori_loop(1, n, greet, 0)

    def take_psi(at):
        return pltpu.make_async_copy(psi_hbm.at[at], psi_ref.at[at], psi_sem.at[at])

    take_pot = pltpu.make_async_copy(pot_hbm, pot_ref, pot_sem)
    take_pot.start()
    for x in range(nx):
        for p in range(2):
            take_psi(p * nx + x).start()

    def remote(src, dst, send_to, recv_to, there):
        return pltpu.make_async_remote_copy(
            src_ref=src, dst_ref=dst, send_sem=send_to, recv_sem=recv_to,
            device_id={"dom": there}, device_id_type=mesh_ids)

    def forward(c, here, there):
        return remote(send.at[c, there], recv.at[c, here + 1], send_sem.at[c, there], recv_sem.at[c, here], there)

    def beside(c, here, there):
        return remote(send.at[c, lax.rem(there + half, n)], extra.at[c, lax.rem(here, half) + 1],
                      extra_send.at[c], extra_recv.at[c, lax.rem(here, half)], there)

    def pot_copy(here, there):
        return remote(pots.at[me], pots.at[here], pot_send, pot_recv.at[here], there)

    def backward(c, owner, there):
        return remote(outb.at[c, there], back.at[c, owner], back_send.at[c], back_recv.at[c, owner], there)

    def far_copy(c, i, there):
        return remote(outx.at[c, i], back.at[c, partner], far_send.at[c], back_recv.at[c, partner], there)

    def note_copy(c):
        return remote(note.at[c], heard.at[c], note_send.at[c], note_recv.at[c], partner)

    def pack(x, carry):
        for p in range(2):
            take_psi(p * nx + x).wait()
        parts = [psi_ref[p * nx + x].T.reshape(n, SUB, LANES) for p in range(2)]
        for c, block in enumerate(interleave(*parts, n)):
            send[c, :, x] = block
        return carry

    lax.fori_loop(0, nx, pack, 0)

    take_pot.wait()
    pots[me] = jnp.concatenate([pot_ref[:, j, :] for j in range(LANES // nz)], axis=1)
    blank = jnp.zeros((nx, SUB, LANES), jnp.float32)
    for c in range(CHUNKS):
        recv[c, me + 1] = send[c, me]
        recv[c, 0] = blank
        recv[c, n + 1] = blank
        extra[c, me - base + 1] = send[c, partner]
        extra[c, 0] = blank
        extra[c, half + 1] = blank
    for j in range(ITERS - 1):
        basis[j, 0] = blank
        basis[j, n + 1] = blank
        inner[j, 0] = blank
        inner[j, half + 1] = blank

    pl.semaphore_wait(barrier, n - 1)

    def send_pot(k, carry):
        pot_copy(me, lax.rem(me + k, n)).start()
        return carry

    lax.fori_loop(1, n, send_pot, 0)

    def sends(c):
        def across(k, carry):
            there = far_plane + lax.rem(spot + k, plane)
            forward(c, me, there).start()
            return carry

        def across_near(k, carry):
            there = plane * (2 - side) + lax.rem(spot + k, plane)
            forward(c, me, there).start()
            return carry

        def home(k, carry):
            forward(c, me, base + lax.rem(me + k, half)).start()
            return carry

        def cross():
            lax.fori_loop(0, plane, across, 0)
            lax.fori_loop(0, plane, across_near, 0)

        def within():
            lax.fori_loop(1, half, home, 0)

        return cross, within

    def send_beside(c):
        def one(k, carry):
            beside(c, me, base + lax.rem(me + k, half)).start()
            return carry

        lax.fori_loop(1, half, one, 0)

    def first_far(k, carry):
        there = far_plane + lax.rem(spot + k, plane)
        forward(0, there, there).wait_recv()
        return carry

    def send_all(c):
        cross, within = sends(c)
        within()
        cross()

    def wait_pot(k, carry):
        there = lax.rem(me + n - k, n)
        pot_copy(there, there).wait_recv()
        return carry

    upper = lax.broadcasted_iota(jnp.int32, (SUB, LANES), 1) >= nz
    lane = lax.broadcasted_iota(jnp.int32, (SUB, LANES), 1)
    sign = jnp.where(lax.broadcasted_iota(jnp.int32, (SUB, LANES), 0) < HALF, 1.0, -1.0)
    ratio = -0.5 * far_weight

    row = lax.broadcasted_iota(jnp.int32, (LANES, LANES), 0)
    column = lax.broadcasted_iota(jnp.int32, (LANES, LANES), 1)
    apart = lax.rem(row - column + 2 * nz, nz)
    near_z = jnp.where(jnp.logical_or(apart == 1, apart == nz - 1), 16.0, 0.0)
    far_z = jnp.where(jnp.logical_or(apart == 2, apart == nz - 2), 1.0, 0.0)
    same = (row < nz) == (column < nz)
    lanes_matrix = jnp.where(same, far_z - near_z, jnp.where(apart == 0, -16.0, 0.0)).astype(jnp.bfloat16)
    mix[0:LANES] = lanes_matrix
    mix[LANES:2 * LANES] = lanes_matrix

    def applied_at(ref, s, slab, size):
        slabs = [[ref[s + g, x] for x in range(nx)] for g in range(size + 2)]
        inside = jnp.concatenate([u for row_of in slabs[1:-1] for u in row_of], axis=0)
        high = inside.astype(jnp.bfloat16)
        rest = (inside - high.astype(jnp.float32)).astype(jnp.bfloat16)
        mixed = jnp.dot(jnp.concatenate([high, rest], axis=1), mix[...], preferred_element_type=jnp.float32)
        result = []
        for g in range(size):
            before, now, after = slabs[g:g + 3]
            for x in range(nx):
                u = now[x]
                close = now[(x + 1) % nx] + now[(x - 1) % nx]
                close = close + pltpu.roll(jnp.where(upper, before[x], after[x]), nz, 1)
                wide = now[(x + 2) % nx] + now[(x - 2) % nx] + before[x] + after[x]
                at = (g * nx + x) * SUB
                wide = wide + mixed[at:at + SUB]
                own = jnp.broadcast_to(pots[slab + g, pl.ds(x, 1), :], (SUB, LANES)) + -0.5 * centre_weight
                result.append((own * u + ratio * (wide - 16.0 * close), u))
        return result

    def blend(us, straight, crossed):
        a = straight[0] * us[0]
        b = crossed[0] * us[0]
        for j in range(1, ITERS):
            a = a + straight[j] * us[j]
            b = b + crossed[j] * us[j]
        return a + swap_parts(b)

    send_all(0)

    @pl.when(inward)
    def _():
        lax.fori_loop(0, plane, first_far, 0)

    send_all(1)
    send_beside(0)
    send_beside(1)

    def chunk(c, carry):
        vectors = [recv.at[c]] + [basis.at[j] for j in range(ITERS - 1)]

        def arrive(k, acc):
            there = lax.rem(me + n - k, n)
            early = jnp.logical_and(there >= far_plane, there < far_plane + plane)
            early = jnp.logical_and(jnp.logical_and(inward, c == 0), early)

            @pl.when(jnp.logical_not(early))
            def _():
                forward(c, there, there).wait_recv()

            for x in range(nx):
                u = recv[c, there + 1, x]
                acc = acc + u * u
            return acc

        acc = jnp.zeros((SUB, LANES), jnp.float32)
        for x in range(nx):
            u = recv[c, me + 1, x]
            acc = acc + u * u
        acc = lax.fori_loop(1, n, arrive, acc)
        first_norm = jnp.sqrt(total_of(acc) + epsilon)

        @pl.when(jnp.logical_and(c > 0, inward))
        def _():
            def held(k, carry):
                backward(c - 1, me, near + lax.rem(me + k, reach)).start()
                return carry

            lax.fori_loop(0, reach, held, 0)

        @pl.when(c == 0)
        def _():
            lax.fori_loop(1, n, wait_pot, 0)

        scales = [1.0 / first_norm]
        alphas, betas, selves, previous = [], [], [], []
        zero = jnp.zeros((SUB, LANES), jnp.float32)
        for j in range(ITERS):
            ref = vectors[j]
            last = j + 1 == ITERS
            fresh = None if last else vectors[j + 1]

            def apply(s, accs, ref=ref, fresh=fresh):
                accs = list(accs)
                for at, (w, u) in enumerate(applied_at(ref, s * GROUP, s * GROUP, GROUP)):
                    if fresh is not None:
                        fresh[s * GROUP + at // nx + 1, at % nx] = w
                    accs[at % 2] = accs[at % 2] + u * w
                return tuple(accs)

            accs = lax.fori_loop(0, n // GROUP, apply, (zero, zero), unroll=UNROLL_A)
            scale = scales[j]
            alpha = scale * (scale * total_of(accs[0] + accs[1]))
            alphas.append(alpha)
            if last:
                break
            by_self = alpha * scale
            by_previous = betas[j - 1] * scales[j - 1] if j else None
            selves.append(by_self)
            previous.append(by_previous)

            def reduce(s, accs, ref=ref, fresh=fresh, scale=scale, by_self=by_self, by_previous=by_previous, j=j):
                accs = list(accs)
                for x in range(nx):
                    r = scale * fresh[s + 1, x] - by_self * ref[s + 1, x]
                    if j:
                        r = r - by_previous * vectors[j - 1][s + 1, x]
                    fresh[s + 1, x] = r
                    accs[x % 2] = accs[x % 2] + r * r
                return tuple(accs)

            accs = lax.fori_loop(0, n, reduce, (zero, zero), unroll=UNROLL_B)
            beta = jnp.sqrt(total_of(accs[0] + accs[1]) + epsilon)
            betas.append(beta)
            scales.append(1.0 / beta)

        real, imag = krylov_weights(alphas, betas)
        straight = [first_norm * scales[j] * real[j] for j in range(ITERS)]
        crossed = [first_norm * scales[j] * imag[j] * sign for j in range(ITERS)]

        told = zero
        for k, value in enumerate(scales[:-1] + selves + previous[1:] + straight + crossed):
            told = jnp.where(lane == k, value, told)
        note[c] = told

        def combined(d, x):
            return blend([v[d + 1, x] for v in vectors], straight, crossed)

        def finish_across(k, carry):
            there = near + lax.rem(me + k, reach)
            for x in range(nx):
                outb[c, there, x] = combined(there, x)

            @pl.when(k == 0)
            def _():
                note_copy(c).start()

            @pl.when(jnp.logical_and(k > 0, jnp.logical_or(c == CHUNKS - 1, jnp.logical_not(inward))))
            def _():
                backward(c, me, near + lax.rem(me + k - 1, reach)).start()

            return carry

        lax.fori_loop(0, reach, finish_across, 0)

        def finish_home(k, carry):
            there = base + lax.rem(me + k, half)
            for x in range(nx):
                outb[c, there, x] = combined(there, x)

            @pl.when(jnp.logical_and(k == 1, jnp.logical_or(c == CHUNKS - 1, jnp.logical_not(inward))))
            def _():
                backward(c, me, near + lax.rem(me + reach - 1, reach)).start()

            @pl.when(k > 1)
            def _():
                backward(c, me, base + lax.rem(me + k - 1, half)).start()

            return carry

        lax.fori_loop(1, half, finish_home, 0)
        for x in range(nx):
            back[c, me, x] = combined(me, x)
        backward(c, me, base + lax.rem(me + half - 1, half)).start()

        return carry

    def assist(c, carry):
        def beside_arrives(k, carry):
            there = base + lax.rem(me + k, half)
            beside(c, there, there).wait_recv()
            return carry

        lax.fori_loop(1, half, beside_arrives, 0)
        note_copy(c).wait_recv()
        words = heard[c]
        word = [jnp.broadcast_to(words[:, k:k + 1], (SUB, LANES)) for k in range(3 * reach - 1 + 2 * ITERS)]
        scales, selves, previous = word[:reach], word[reach:2 * reach], [None] + word[2 * reach:3 * reach - 1]
        straight, crossed = word[3 * reach - 1:3 * reach - 1 + ITERS], word[3 * reach - 1 + ITERS:]

        halves = [extra.at[c]] + [inner.at[j] for j in range(reach)]
        for j in range(reach):
            count = half - 1 - j
            start = (j + 1) * side
            pieces = -(-count // GROUP)
            at = 0
            for piece in range(pieces):
                size = (count - at) // (pieces - piece)
                for i, (w, u) in enumerate(applied_at(halves[j], start + at, base + start + at, size)):
                    here = start + at + i // nx + 1
                    r = scales[j] * w - selves[j] * u
                    if j:
                        r = r - previous[j] * halves[j - 1][here, i % nx]
                    halves[j + 1][here, i % nx] = r
                at += size

        first = reach * side
        for i in range(deep):
            for x in range(nx):
                outx[c, i, x] = blend([v[first + i + 1, x] for v in halves], straight, crossed)
        for i in range(deep):
            there = base + first + i

            @pl.when(there == me)
            def _(i=i):
                back[c, partner] = outx[c, i]

            @pl.when(there != me)
            def _(i=i, there=there):
                far_copy(c, i, there).start()

        return carry

    lax.fori_loop(0, CHUNKS, chunk, 0)
    lax.fori_loop(0, CHUNKS, assist, 0)

    remote(pots.at[pl.ds(0, n - 1)], pots.at[pl.ds(0, n - 1)], pot_send, pot_recv.at[0], partner).wait_send()
    def sent(k, carry):
        for c in range(CHUNKS):
            forward(c, me, lax.rem(me + k, n)).wait_send()
        return carry

    lax.fori_loop(1, n, sent, 0)
    for c in range(CHUNKS):
        blocks = send.at[c, pl.ds(0, half - 1)]
        remote(blocks, blocks, extra_send.at[c], recv_sem.at[c, 0], partner).wait_send()
        note_copy(c).wait_send()

    for c in range(CHUNKS):
        def returned(k, carry, c=c):
            there = lax.rem(me + n - k, n)

            @pl.when(jnp.logical_not(jnp.logical_and(outer, there == partner)))
            def _():
                backward(c, there, there).wait_recv()

            return carry

        lax.fori_loop(1, n, returned, 0)

    for c in range(CHUNKS):
        blocks = outb.at[c, pl.ds(0, reach + half - 1)]
        remote(blocks, blocks, back_send.at[c], recv_sem.at[c, 0], partner).wait_send()

        @pl.when(outer)
        def _(c=c):
            blocks = outx.at[c, pl.ds(0, deep - 1)]
            remote(blocks, blocks, far_send.at[c], recv_sem.at[c, 0], partner).wait_send()

        @pl.when(jnp.logical_not(outer))
        def _(c=c):
            blocks = outx.at[c]
            remote(blocks, blocks, far_send.at[c], recv_sem.at[c, 0], partner).wait_send()


def fused(psi, potential, n):
    parts, slabs, nx, by, nz, orbs = psi.shape
    half, reach = n // 2, ITERS - 1
    vec = lambda *lead: pltpu.VMEM(lead + (nx, SUB, LANES), jnp.float32)
    tile = lambda *lead: pltpu.VMEM(lead + (SUB, LANES), jnp.float32)
    dma = lambda *shape: pltpu.SemaphoreType.DMA(shape)
    result = pl.pallas_call(
        functools.partial(kernel, n, nx, nz),
        out_shape=pltpu.VMEM((CHUNKS, n, nx, SUB, LANES), jnp.float32),
        in_specs=[pl.BlockSpec(memory_space=pl.ANY)] * 2,
        out_specs=pl.BlockSpec(memory_space=pltpu.VMEM),
        scratch_shapes=[
            pltpu.VMEM((parts * nx, by * nz, orbs), jnp.float32), pltpu.VMEM((nx, by, nz), jnp.float32),
            vec(CHUNKS, n), vec(CHUNKS, n + 2), vec(CHUNKS, half + 2), vec(reach, n + 2), vec(reach, half + 2),
            vec(CHUNKS, n), vec(CHUNKS, half - reach),
            pltpu.VMEM((n, nx, LANES), jnp.float32), pltpu.VMEM((2 * LANES, LANES), jnp.bfloat16),
            tile(CHUNKS), tile(CHUNKS),
            dma(CHUNKS, n), dma(CHUNKS, n), dma(CHUNKS), dma(CHUNKS, half), pltpu.SemaphoreType.DMA, dma(n),
            dma(CHUNKS), dma(CHUNKS, n), dma(CHUNKS), dma(CHUNKS), dma(CHUNKS), dma(parts * nx), dma(),
        ],
        compiler_params=pltpu.CompilerParams(collective_id=0, has_side_effects=True),
    )(psi.reshape(parts * nx, by * nz, orbs), potential.reshape(nx, by, nz))
    out = pl.pallas_call(
        functools.partial(unpack_kernel, n, nx),
        out_shape=jax.ShapeDtypeStruct((parts * nx, by * nz, orbs), jnp.float32),
        in_specs=[pl.BlockSpec(memory_space=pltpu.VMEM)],
        out_specs=pl.BlockSpec(memory_space=pl.ANY),
        scratch_shapes=[pltpu.VMEM((parts * nx, by * nz, orbs), jnp.float32), dma(parts * nx)],
    )(pltpu.with_memory_space_constraint(result, pltpu.VMEM))
    return out.reshape(psi.shape)


def fits(psi, n):
    parts, slabs, nx, by, nz, orbs = psi.shape
    return parts == 2 and slabs == 1 and by == 2 and by * nz == LANES and orbs == LANES and orbs == n * SUB and n % GROUP == 0 and n // 2 > ITERS


def per_device(n, psi, potential):
    if fits(psi, n):
        return fused(psi, potential, n)
    return on_device(psi, potential)


def solution(mesh):
    placed = (P(None, "dom", None, None, None, "st"), P("dom", None, None, None))
    return jax.shard_map(
        functools.partial(per_device, mesh.shape["dom"]),
        mesh=mesh,
        in_specs=placed,
        out_specs=P(None, "dom", None, None, None, "st"),
        check_vma=False,
    )
```

```python
import functools

import jax
import jax.numpy as jnp
from jax import lax
from jax.experimental import pallas as pl
from jax.experimental.pallas import tpu as pltpu
from jax.sharding import PartitionSpec as P

ITERS = 6


epsilon = 1e-06
time_step = 0.5
taylor_terms = 32
far_weight = -1.0 / 12.0
near_weight = 4.0 / 3.0
centre_weight = -7.5


def to_grid(blocked):
    parts, nblocks, cx, by, nz, orbs = blocked.shape
    grid = blocked.transpose(0, 2, 1, 3, 4, 5)
    return grid.reshape(parts, cx, nblocks * by, nz, orbs)


def to_blocks(grid, by):
    parts, nx, ny, nz, orbs = grid.shape
    blocked = grid.reshape(parts, nx, ny // by, by, nz, orbs).transpose(0, 2, 1, 3, 4, 5)
    return blocked


def shift_walls(values, offset):
    width_y = values.shape[2]
    padded = jnp.pad(values, ((0, 0), (0, 0), (2, 2), (0, 0), (0, 0)))
    return padded[:, :, 2 - offset : 2 - offset + width_y]


def hamiltonian_whole(values_in, potential):
    total = centre_weight * values_in
    for along in (1, 3):
        total = total + near_weight * (
            jnp.roll(values_in, 1, along) + jnp.roll(values_in, -1, along)
        )
        total = total + far_weight * (
            jnp.roll(values_in, 2, along) + jnp.roll(values_in, -2, along)
        )
    total = total + near_weight * (shift_walls(values_in, 1) + shift_walls(values_in, -1))
    total = total + far_weight * (shift_walls(values_in, 2) + shift_walls(values_in, -2))
    return -0.5 * total + potential[None, :, :, :, None] * values_in


def tridiagonal(alphas, betas, vector):
    zero_row = jnp.zeros((1, vector.shape[1]), jnp.float32)
    upper = jnp.concatenate([betas * vector[1:], zero_row], axis=0)
    lower = jnp.concatenate([zero_row, betas * vector[:-1]], axis=0)
    return alphas * vector + upper + lower


def krylov_exponential(alphas, betas):
    count = alphas.shape[0]
    first = (jnp.arange(count) == 0).astype(jnp.float32)[:, None] * jnp.ones_like(alphas)
    term_real = first
    term_imag = jnp.zeros_like(alphas)
    sum_real = term_real
    sum_imag = term_imag
    for order in range(1, taylor_terms):
        applied_real = tridiagonal(alphas, betas, term_real)
        applied_imag = tridiagonal(alphas, betas, term_imag)
        term_real = time_step * applied_imag / order
        term_imag = -time_step * applied_real / order
        sum_real = sum_real + term_real
        sum_imag = sum_imag + term_imag
    return (sum_real, sum_imag)


def combine_basis(krylov_basis, alpha_list, beta_list, first_norm):
    coef_real, coef_imag = krylov_exponential(jnp.stack(alpha_list), jnp.stack(beta_list))
    out_real = jnp.zeros_like(krylov_basis[0][0])
    out_imag = jnp.zeros_like(krylov_basis[0][0])
    for index_j in range(len(krylov_basis)):
        basis_now = krylov_basis[index_j]
        out_real = out_real + coef_real[index_j] * basis_now[0] - coef_imag[index_j] * basis_now[1]
        out_imag = out_imag + coef_real[index_j] * basis_now[1] + coef_imag[index_j] * basis_now[0]
    return first_norm * jnp.stack([out_real, out_imag])


def local_lanczos(grid_psi, grid_pot):
    axes_all = (0, 1, 2, 3)
    first_norm = jnp.sqrt(jnp.sum(grid_psi * grid_psi, axis=axes_all) + epsilon)
    vector = grid_psi / first_norm
    previous = jnp.zeros_like(vector)
    beta_prev = jnp.zeros_like(first_norm)
    krylov_basis = []
    alpha_list = []
    beta_list = []
    for iteration in range(ITERS):
        applied = hamiltonian_whole(vector, grid_pot)
        alpha_now = jnp.sum(vector * applied, axis=axes_all)
        krylov_basis.append(vector)
        alpha_list.append(alpha_now)
        if iteration + 1 < ITERS:
            remainder = applied - alpha_now * vector - beta_prev * previous
            beta_now = jnp.sqrt(jnp.sum(remainder * remainder, axis=axes_all) + epsilon)
            previous = vector
            vector = remainder / beta_now
            beta_prev = beta_now
            beta_list.append(beta_now)
    return combine_basis(krylov_basis, alpha_list, beta_list, first_norm)


def on_device(psi, potential):
    by = psi.shape[3]
    moved = lax.all_to_all(psi, "dom", split_axis=5, concat_axis=1, tiled=True)
    whole_pot = lax.all_gather(potential, "dom", axis=0, tiled=True)
    grid_pot = to_grid(whole_pot[None, :, :, :, :, None])[0, :, :, :, 0]
    result = to_blocks(local_lanczos(to_grid(moved), grid_pot), by)
    return lax.all_to_all(result, "dom", split_axis=1, concat_axis=5, tiled=True)


SUB = 8
LANES = 128
HALF = SUB // 2
CHUNKS = 2
GROUP = 4


def swap_parts(x):
    return pltpu.roll(x, HALF, 0)


def total_of(acc):
    summed = jnp.broadcast_to(jnp.sum(acc, axis=1, keepdims=True), (SUB, LANES))
    return summed + swap_parts(summed)


def krylov_weights(alphas, betas):
    count = len(alphas)
    one = jnp.ones((SUB, LANES), jnp.float32)
    term = [one] + [None] * (count - 1)
    real = [one] + [None] * (count - 1)
    imag = [None] * count
    for order in range(1, taylor_terms):
        fresh = []
        for i in range(count):
            pieces = []
            if term[i] is not None:
                pieces.append(alphas[i] * term[i])
            if i + 1 < count and term[i + 1] is not None:
                pieces.append(betas[i] * term[i + 1])
            if i > 0 and term[i - 1] is not None:
                pieces.append(betas[i - 1] * term[i - 1])
            fresh.append(sum(pieces[1:], pieces[0]) * (time_step / order) if pieces else None)
        term = fresh
        into = imag if order % 2 else real
        minus = order % 4 in (1, 2)
        for i in range(count):
            if term[i] is not None:
                if into[i] is None:
                    into[i] = -term[i] if minus else term[i]
                else:
                    into[i] = into[i] - term[i] if minus else into[i] + term[i]
    zero = jnp.zeros((SUB, LANES), jnp.float32)
    return [zero if r is None else r for r in real], [zero if m is None else m for m in imag]


def interleave(a, b, n):
    low = lax.broadcasted_iota(jnp.int32, (n, SUB, LANES), 1) < HALF
    return (jnp.where(low, a, pltpu.roll(b, HALF, 1)), jnp.where(low, pltpu.roll(a, HALF, 1), b))


def unpack_kernel(n, nx, back, out_hbm, out, sems):
    def put(at):
        return pltpu.make_async_copy(out.at[at], out_hbm.at[at], sems.at[at])

    for x in range(nx):
        for p, block in enumerate(interleave(back[0, :, x], back[1, :, x], n)):
            out[p * nx + x] = block.reshape(n * SUB, LANES).T
        if x:
            for p in range(2):
                put(p * nx + x - 1).start()
    for p in range(2):
        put(p * nx + nx - 1).start()
    for at in range(2 * nx):
        put(at).wait()


def kernel(n, nx, nz, psi_hbm, pot_hbm, back, psi_ref, pot_ref, send, recv, extra, basis, inner, outb, outx, pots, mix,
           note, heard, send_sem, recv_sem, extra_send, extra_recv, pot_send, pot_recv, back_send, back_recv,
           far_send, note_send, note_recv, psi_sem, pot_sem, held):
    me = lax.axis_index("dom")
    mesh_ids = pl.DeviceIdType.MESH
    barrier = pltpu.get_barrier_semaphore()

    ratio = -0.5 * far_weight
    half = n // 2
    reach = ITERS - 1
    deep = half - reach
    side = me // half
    base = side * half
    opposite = half - base
    partner = lax.rem(me + half, n)
    near = half - side * reach
    outer = jnp.logical_or(me < deep, me >= n - deep)
    plane = n // 4
    spot = lax.rem(me, plane)
    inward = jnp.logical_and(me >= plane, me < n - plane)
    far_plane = (1 - side) * (n - plane)

    def greet(k, carry):
        pl.semaphore_signal(barrier, inc=1, device_id={"dom": lax.rem(me + k, n)}, device_id_type=mesh_ids)
        return carry

    lax.fori_loop(1, n, greet, 0)

    def take_psi(at):
        return pltpu.make_async_copy(psi_hbm.at[at], psi_ref.at[at], psi_sem.at[at])

    take_pot = pltpu.make_async_copy(pot_hbm, pot_ref, pot_sem)
    take_pot.start()
    for x in range(nx):
        for p in range(2):
            take_psi(p * nx + x).start()

    def remote(src, dst, send_to, recv_to, there):
        return pltpu.make_async_remote_copy(
            src_ref=src, dst_ref=dst, send_sem=send_to, recv_sem=recv_to,
            device_id={"dom": there}, device_id_type=mesh_ids)

    def forward(c, here, there):
        return remote(send.at[c, there], recv.at[c, here + 1], send_sem.at[c, there], recv_sem.at[c, here], there)

    def beside(c, here, there):
        return remote(send.at[c, lax.rem(there + half, n)], extra.at[c, lax.rem(here, half) + 1],
                      extra_send.at[c], extra_recv.at[c, lax.rem(here, half)], there)

    def pot_copy(here, there):
        return remote(pots.at[me], pots.at[here], pot_send, pot_recv.at[here], there)

    def backward(c, owner, there):
        return remote(outb.at[c, there], back.at[c, owner], back_send.at[c], back_recv.at[c, owner], there)

    def far_copy(c, i, there):
        return remote(outx.at[c, i], back.at[c, partner], far_send.at[c], back_recv.at[c, partner], there)

    def note_copy(c):
        return remote(note.at[c], heard.at[c], note_send.at[c], note_recv.at[c], partner)

    def pack(x, carry):
        for p in range(2):
            take_psi(p * nx + x).wait()
        parts = [psi_ref[p * nx + x].T.reshape(n, SUB, LANES) for p in range(2)]
        for c, block in enumerate(interleave(*parts, n)):
            send[c, :, x] = block
        return carry

    lax.fori_loop(0, nx, pack, 0, unroll=4)

    take_pot.wait()
    pot_rows = jnp.concatenate([pot_ref[:, j, :] for j in range(LANES // nz)], axis=1)
    pots[me] = (pot_rows + -0.5 * centre_weight) * (1.0 / ratio)
    blank = jnp.zeros((nx, SUB, LANES), jnp.float32)
    for c in range(CHUNKS):
        recv[c, me + 1] = send[c, me]
        recv[c, 0] = blank
        recv[c, n + 1] = blank
        extra[c, me - base + 1] = send[c, partner]
        extra[c, 0] = blank
        extra[c, half + 1] = blank
    for j in range(ITERS - 1):
        basis[j, 0] = blank
        basis[j, n + 1] = blank
        inner[j, 0] = blank
        inner[j, half + 1] = blank

    pl.semaphore_wait(barrier, n - 1)

    def send_pot(k, carry):
        pot_copy(me, lax.rem(me + k, n)).start()
        return carry

    lax.fori_loop(1, n, send_pot, 0)

    def sends(c):
        def across(k, carry):
            there = far_plane + lax.rem(spot + k, plane)
            forward(c, me, there).start()
            return carry

        def across_near(k, carry):
            there = plane * (2 - side) + lax.rem(spot + k, plane)
            forward(c, me, there).start()
            return carry

        def home(k, carry):
            forward(c, me, base + lax.rem(me + k, half)).start()
            return carry

        def cross():
            lax.fori_loop(0, plane, across, 0)
            lax.fori_loop(0, plane, across_near, 0)

        def within():
            lax.fori_loop(1, half, home, 0)

        return cross, within

    def send_beside(c):
        def one(k, carry):
            beside(c, me, base + lax.rem(me + k, half)).start()
            return carry

        lax.fori_loop(1, half, one, 0)

    def first_far(k, carry):
        there = far_plane + lax.rem(spot + k, plane)
        forward(0, there, there).wait_recv()
        return carry

    def send_all(c):
        cross, within = sends(c)
        within()
        cross()

    def wait_pot(k, carry):
        there = lax.rem(me + n - k, n)
        pot_copy(there, there).wait_recv()
        return carry

    upper = lax.broadcasted_iota(jnp.int32, (SUB, LANES), 1) >= nz
    lane = lax.broadcasted_iota(jnp.int32, (SUB, LANES), 1)
    sign = jnp.where(lax.broadcasted_iota(jnp.int32, (SUB, LANES), 0) < HALF, 1.0, -1.0)

    row = lax.broadcasted_iota(jnp.int32, (LANES, LANES), 0)
    column = lax.broadcasted_iota(jnp.int32, (LANES, LANES), 1)
    apart = lax.rem(row - column + 2 * nz, nz)
    near_z = jnp.where(jnp.logical_or(apart == 1, apart == nz - 1), 16.0, 0.0)
    far_z = jnp.where(jnp.logical_or(apart == 2, apart == nz - 2), 1.0, 0.0)
    same = (row < nz) == (column < nz)
    lanes_matrix = jnp.where(same, far_z - near_z, jnp.where(apart == 0, -16.0, 0.0)).astype(jnp.bfloat16)
    mix[0:LANES] = lanes_matrix
    mix[LANES:2 * LANES] = lanes_matrix

    def applied_at(ref, s, slab, size):
        slabs = [[ref[s + g, x] for x in range(nx)] for g in range(size + 2)]
        inside = jnp.concatenate([u for row_of in slabs[1:-1] for u in row_of], axis=0)
        high = inside.astype(jnp.bfloat16)
        rest = (inside - high.astype(jnp.float32)).astype(jnp.bfloat16)
        mixed = jnp.dot(jnp.concatenate([high, rest], axis=1), mix[...], preferred_element_type=jnp.float32)
        result = []
        for g in range(size):
            before, now, after = slabs[g:g + 3]
            for x in range(nx):
                u = now[x]
                close = now[(x + 1) % nx] + now[(x - 1) % nx]
                close = close + pltpu.roll(jnp.where(upper, before[x], after[x]), nz, 1)
                wide = now[(x + 2) % nx] + now[(x - 2) % nx] + before[x] + after[x]
                at = (g * nx + x) * SUB
                wide = wide + mixed[at:at + SUB]
                own = jnp.broadcast_to(pots[slab + g, pl.ds(x, 1), :], (SUB, LANES))
                result.append((own * u + (wide - 16.0 * close), u))
        return result

    def blend(us, straight, crossed):
        a = straight[0] * us[0]
        b = crossed[0] * us[0]
        for j in range(1, ITERS):
            a = a + straight[j] * us[j]
            b = b + crossed[j] * us[j]
        return a + swap_parts(b)

    send_all(0)

    @pl.when(inward)
    def _():
        lax.fori_loop(0, plane, first_far, 0)

    send_all(1)
    send_beside(0)
    send_beside(1)

    def chunk(c, carry):
        vectors = [recv.at[c]] + [basis.at[j] for j in range(ITERS - 1)]

        def arrive(k, acc):
            there = lax.rem(me + n - k, n)
            early = jnp.logical_and(there >= far_plane, there < far_plane + plane)
            early = jnp.logical_and(jnp.logical_and(inward, c == 0), early)

            @pl.when(jnp.logical_not(early))
            def _():
                forward(c, there, there).wait_recv()

            for x in range(nx):
                u = recv[c, there + 1, x]
                acc = acc + u * u
            return acc

        acc = jnp.zeros((SUB, LANES), jnp.float32)
        for x in range(nx):
            u = recv[c, me + 1, x]
            acc = acc + u * u
        acc = lax.fori_loop(1, n, arrive, acc)
        square = total_of(acc) + epsilon
        scale = lax.rsqrt(square)
        first_norm = square * scale

        @pl.when(jnp.logical_and(c > 0, inward))
        def _():
            def kept(k, carry):
                backward(c - 1, me, near + lax.rem(me + k, reach)).start()
                return carry

            del kept

        @pl.when(c == 0)
        def _():
            lax.fori_loop(1, n, wait_pot, 0)

        scales, steps = [scale], []
        alphas, betas, selves, previous = [], [], [], []
        zero = jnp.zeros((SUB, LANES), jnp.float32)
        for j in range(ITERS):
            ref = vectors[j]
            products = [zero, zero]
            squares = [zero, zero]
            done = 0
            for g in range(n // GROUP + 1):
                if j and g < n // GROUP:
                    for s in range(g * GROUP, (g + 1) * GROUP):
                        for x in range(nx):
                            r = steps[-1] * held[(j - 1) % 2, s, x] - selves[-1] * vectors[j - 1][s + 1, x]
                            if j > 1:
                                r = r - previous[-1] * vectors[j - 2][s + 1, x]
                            ref[s + 1, x] = r
                            squares[x % 2] = squares[x % 2] + r * r
                if j and g == n // GROUP:
                    square = total_of(squares[0] + squares[1]) + epsilon
                upto = n if g == n // GROUP else (g + 1) * GROUP - 1
                for at, (w, u) in enumerate(applied_at(ref, done, done, upto - done)):
                    if j + 1 < ITERS:
                        held[j % 2, done + at // nx, at % nx] = w
                    products[at % 2] = products[at % 2] + u * w
                done = upto
            if j:
                scale = lax.rsqrt(square)
                scales.append(scale)
                betas.append(square * scale)
            step = scale * ratio
            alpha = step * (scale * total_of(products[0] + products[1]))
            alphas.append(alpha)
            if j + 1 < ITERS:
                steps.append(step)
                selves.append(alpha * scale)
                previous.append(betas[-1] * scales[-2] if j else None)

        real, imag = krylov_weights(alphas, betas)
        straight = [first_norm * scales[j] * real[j] for j in range(ITERS)]
        crossed = [first_norm * scales[j] * imag[j] * sign for j in range(ITERS)]

        told = zero
        for k, value in enumerate(steps + selves + previous[1:] + straight + crossed):
            told = jnp.where(lane == k, value, told)
        note[c] = told

        def combined(d, x):
            return blend([v[d + 1, x] for v in vectors], straight, crossed)

        def finish_across(k, carry):
            there = near + lax.rem(me + k, reach)
            for x in range(nx):
                outb[c, there, x] = combined(there, x)

            @pl.when(k == 0)
            def _():
                note_copy(c).start()

            @pl.when(jnp.logical_and(k == 1, jnp.logical_and(c > 0, inward)))
            def _():
                def late(i, carry):
                    backward(c - 1, me, near + lax.rem(me + i, reach)).start()
                    return carry

                lax.fori_loop(0, reach, late, 0)

            @pl.when(jnp.logical_and(k > 0, jnp.logical_or(c == CHUNKS - 1, jnp.logical_not(inward))))
            def _():
                backward(c, me, near + lax.rem(me + k - 1, reach)).start()

            return carry

        lax.fori_loop(0, reach, finish_across, 0)

        def finish_home(k, carry):
            there = base + lax.rem(me + k, half)
            for x in range(nx):
                outb[c, there, x] = combined(there, x)

            @pl.when(jnp.logical_and(k == 1, jnp.logical_or(c == CHUNKS - 1, jnp.logical_not(inward))))
            def _():
                backward(c, me, near + lax.rem(me + reach - 1, reach)).start()

            @pl.when(k > 1)
            def _():
                backward(c, me, base + lax.rem(me + k - 1, half)).start()

            return carry

        lax.fori_loop(1, half, finish_home, 0)
        for x in range(nx):
            back[c, me, x] = combined(me, x)
        backward(c, me, base + lax.rem(me + half - 1, half)).start()

        return carry

    def assist(c, carry):
        def beside_arrives(k, carry):
            there = base + lax.rem(me + k, half)
            beside(c, there, there).wait_recv()
            return carry

        lax.fori_loop(1, half, beside_arrives, 0)
        note_copy(c).wait_recv()
        words = heard[c]
        word = [jnp.broadcast_to(words[:, k:k + 1], (SUB, LANES)) for k in range(3 * reach - 1 + 2 * ITERS)]
        steps, selves, previous = word[:reach], word[reach:2 * reach], [None] + word[2 * reach:3 * reach - 1]
        straight, crossed = word[3 * reach - 1:3 * reach - 1 + ITERS], word[3 * reach - 1 + ITERS:]

        halves = [extra.at[c]] + [inner.at[j] for j in range(reach)]
        for j in range(reach):
            count = half - 1 - j
            start = (j + 1) * side
            pieces = -(-count // GROUP)
            at = 0
            for piece in range(pieces):
                size = (count - at) // (pieces - piece)
                for i, (w, u) in enumerate(applied_at(halves[j], start + at, base + start + at, size)):
                    here = start + at + i // nx + 1
                    r = steps[j] * w - selves[j] * u
                    if j:
                        r = r - previous[j] * halves[j - 1][here, i % nx]
                    halves[j + 1][here, i % nx] = r
                at += size

        first = reach * side
        for i in range(deep):
            for x in range(nx):
                outx[c, i, x] = blend([v[first + i + 1, x] for v in halves], straight, crossed)
        for i in range(deep):
            there = base + first + i

            @pl.when(there == me)
            def _(i=i):
                back[c, partner] = outx[c, i]

            @pl.when(there != me)
            def _(i=i, there=there):
                far_copy(c, i, there).start()

        return carry

    lax.fori_loop(0, CHUNKS, chunk, 0)
    lax.fori_loop(0, CHUNKS, assist, 0)

    remote(pots.at[pl.ds(0, n - 1)], pots.at[pl.ds(0, n - 1)], pot_send, pot_recv.at[0], partner).wait_send()
    def sent(k, carry):
        for c in range(CHUNKS):
            forward(c, me, lax.rem(me + k, n)).wait_send()
        return carry

    lax.fori_loop(1, n, sent, 0)
    for c in range(CHUNKS):
        blocks = send.at[c, pl.ds(0, half - 1)]
        remote(blocks, blocks, extra_send.at[c], recv_sem.at[c, 0], partner).wait_send()
        note_copy(c).wait_send()

    for c in range(CHUNKS):
        def returned(k, carry, c=c):
            there = lax.rem(me + n - k, n)

            @pl.when(jnp.logical_not(jnp.logical_and(outer, there == partner)))
            def _():
                backward(c, there, there).wait_recv()

            return carry

        lax.fori_loop(1, n, returned, 0)

    for c in range(CHUNKS):
        blocks = outb.at[c, pl.ds(0, reach + half - 1)]
        remote(blocks, blocks, back_send.at[c], recv_sem.at[c, 0], partner).wait_send()

        @pl.when(outer)
        def _(c=c):
            blocks = outx.at[c, pl.ds(0, deep - 1)]
            remote(blocks, blocks, far_send.at[c], recv_sem.at[c, 0], partner).wait_send()

        @pl.when(jnp.logical_not(outer))
        def _(c=c):
            blocks = outx.at[c]
            remote(blocks, blocks, far_send.at[c], recv_sem.at[c, 0], partner).wait_send()


def fused(psi, potential, n):
    parts, slabs, nx, by, nz, orbs = psi.shape
    half, reach = n // 2, ITERS - 1
    vec = lambda *lead: pltpu.VMEM(lead + (nx, SUB, LANES), jnp.float32)
    tile = lambda *lead: pltpu.VMEM(lead + (SUB, LANES), jnp.float32)
    dma = lambda *shape: pltpu.SemaphoreType.DMA(shape)
    result = pl.pallas_call(
        functools.partial(kernel, n, nx, nz),
        out_shape=pltpu.VMEM((CHUNKS, n, nx, SUB, LANES), jnp.float32),
        in_specs=[pl.BlockSpec(memory_space=pl.ANY)] * 2,
        out_specs=pl.BlockSpec(memory_space=pltpu.VMEM),
        scratch_shapes=[
            pltpu.VMEM((parts * nx, by * nz, orbs), jnp.float32), pltpu.VMEM((nx, by, nz), jnp.float32),
            vec(CHUNKS, n), vec(CHUNKS, n + 2), vec(CHUNKS, half + 2), vec(reach, n + 2), vec(reach, half + 2),
            vec(CHUNKS, n), vec(CHUNKS, half - reach),
            pltpu.VMEM((n, nx, LANES), jnp.float32), pltpu.VMEM((2 * LANES, LANES), jnp.bfloat16),
            tile(CHUNKS), tile(CHUNKS),
            dma(CHUNKS, n), dma(CHUNKS, n), dma(CHUNKS), dma(CHUNKS, half), pltpu.SemaphoreType.DMA, dma(n),
            dma(CHUNKS), dma(CHUNKS, n), dma(CHUNKS), dma(CHUNKS), dma(CHUNKS), dma(parts * nx), dma(), vec(2, n),
        ],
        compiler_params=pltpu.CompilerParams(collective_id=0, has_side_effects=True),
    )(psi.reshape(parts * nx, by * nz, orbs), potential.reshape(nx, by, nz))
    out = pl.pallas_call(
        functools.partial(unpack_kernel, n, nx),
        out_shape=jax.ShapeDtypeStruct((parts * nx, by * nz, orbs), jnp.float32),
        in_specs=[pl.BlockSpec(memory_space=pltpu.VMEM)],
        out_specs=pl.BlockSpec(memory_space=pl.ANY),
        scratch_shapes=[pltpu.VMEM((parts * nx, by * nz, orbs), jnp.float32), dma(parts * nx)],
    )(pltpu.with_memory_space_constraint(result, pltpu.VMEM))
    return out.reshape(psi.shape)


def fits(psi, n):
    parts, slabs, nx, by, nz, orbs = psi.shape
    return parts == 2 and slabs == 1 and by == 2 and by * nz == LANES and orbs == LANES and orbs == n * SUB and n % GROUP == 0 and n // 2 > ITERS


def per_device(n, psi, potential):
    if fits(psi, n):
        return fused(psi, potential, n)
    return on_device(psi, potential)


def solution(mesh):
    placed = (P(None, "dom", None, None, None, "st"), P("dom", None, None, None))
    return jax.shard_map(
        functools.partial(per_device, mesh.shape["dom"]),
        mesh=mesh,
        in_specs=placed,
        out_specs=P(None, "dom", None, None, None, "st"),
        check_vma=False,
    )
```

```python
import functools

import jax
import jax.numpy as jnp
from jax import lax
from jax.experimental import pallas as pl
from jax.experimental.pallas import tpu as pltpu
from jax.sharding import PartitionSpec as P

ITERS = 6


epsilon = 1e-06
time_step = 0.5
taylor_terms = 32
far_weight = -1.0 / 12.0
near_weight = 4.0 / 3.0
centre_weight = -7.5


def to_grid(blocked):
    parts, nblocks, cx, by, nz, orbs = blocked.shape
    grid = blocked.transpose(0, 2, 1, 3, 4, 5)
    return grid.reshape(parts, cx, nblocks * by, nz, orbs)


def to_blocks(grid, by):
    parts, nx, ny, nz, orbs = grid.shape
    blocked = grid.reshape(parts, nx, ny // by, by, nz, orbs).transpose(0, 2, 1, 3, 4, 5)
    return blocked


def shift_walls(values, offset):
    width_y = values.shape[2]
    padded = jnp.pad(values, ((0, 0), (0, 0), (2, 2), (0, 0), (0, 0)))
    return padded[:, :, 2 - offset : 2 - offset + width_y]


def hamiltonian_whole(values_in, potential):
    total = centre_weight * values_in
    for along in (1, 3):
        total = total + near_weight * (
            jnp.roll(values_in, 1, along) + jnp.roll(values_in, -1, along)
        )
        total = total + far_weight * (
            jnp.roll(values_in, 2, along) + jnp.roll(values_in, -2, along)
        )
    total = total + near_weight * (shift_walls(values_in, 1) + shift_walls(values_in, -1))
    total = total + far_weight * (shift_walls(values_in, 2) + shift_walls(values_in, -2))
    return -0.5 * total + potential[None, :, :, :, None] * values_in


def tridiagonal(alphas, betas, vector):
    zero_row = jnp.zeros((1, vector.shape[1]), jnp.float32)
    upper = jnp.concatenate([betas * vector[1:], zero_row], axis=0)
    lower = jnp.concatenate([zero_row, betas * vector[:-1]], axis=0)
    return alphas * vector + upper + lower


def krylov_exponential(alphas, betas):
    count = alphas.shape[0]
    first = (jnp.arange(count) == 0).astype(jnp.float32)[:, None] * jnp.ones_like(alphas)
    term_real = first
    term_imag = jnp.zeros_like(alphas)
    sum_real = term_real
    sum_imag = term_imag
    for order in range(1, taylor_terms):
        applied_real = tridiagonal(alphas, betas, term_real)
        applied_imag = tridiagonal(alphas, betas, term_imag)
        term_real = time_step * applied_imag / order
        term_imag = -time_step * applied_real / order
        sum_real = sum_real + term_real
        sum_imag = sum_imag + term_imag
    return (sum_real, sum_imag)


def combine_basis(krylov_basis, alpha_list, beta_list, first_norm):
    coef_real, coef_imag = krylov_exponential(jnp.stack(alpha_list), jnp.stack(beta_list))
    out_real = jnp.zeros_like(krylov_basis[0][0])
    out_imag = jnp.zeros_like(krylov_basis[0][0])
    for index_j in range(len(krylov_basis)):
        basis_now = krylov_basis[index_j]
        out_real = out_real + coef_real[index_j] * basis_now[0] - coef_imag[index_j] * basis_now[1]
        out_imag = out_imag + coef_real[index_j] * basis_now[1] + coef_imag[index_j] * basis_now[0]
    return first_norm * jnp.stack([out_real, out_imag])


def local_lanczos(grid_psi, grid_pot):
    axes_all = (0, 1, 2, 3)
    first_norm = jnp.sqrt(jnp.sum(grid_psi * grid_psi, axis=axes_all) + epsilon)
    vector = grid_psi / first_norm
    previous = jnp.zeros_like(vector)
    beta_prev = jnp.zeros_like(first_norm)
    krylov_basis = []
    alpha_list = []
    beta_list = []
    for iteration in range(ITERS):
        applied = hamiltonian_whole(vector, grid_pot)
        alpha_now = jnp.sum(vector * applied, axis=axes_all)
        krylov_basis.append(vector)
        alpha_list.append(alpha_now)
        if iteration + 1 < ITERS:
            remainder = applied - alpha_now * vector - beta_prev * previous
            beta_now = jnp.sqrt(jnp.sum(remainder * remainder, axis=axes_all) + epsilon)
            previous = vector
            vector = remainder / beta_now
            beta_prev = beta_now
            beta_list.append(beta_now)
    return combine_basis(krylov_basis, alpha_list, beta_list, first_norm)


def on_device(psi, potential):
    by = psi.shape[3]
    moved = lax.all_to_all(psi, "dom", split_axis=5, concat_axis=1, tiled=True)
    whole_pot = lax.all_gather(potential, "dom", axis=0, tiled=True)
    grid_pot = to_grid(whole_pot[None, :, :, :, :, None])[0, :, :, :, 0]
    result = to_blocks(local_lanczos(to_grid(moved), grid_pot), by)
    return lax.all_to_all(result, "dom", split_axis=1, concat_axis=5, tiled=True)


SUB = 8
LANES = 128
HALF = SUB // 2
CHUNKS = 2
GROUP = 4


def swap_parts(x):
    return pltpu.roll(x, HALF, 0)


def total_of(acc):
    summed = jnp.broadcast_to(jnp.sum(acc, axis=1, keepdims=True), (SUB, LANES))
    return summed + swap_parts(summed)


def krylov_weights(alphas, betas):
    count = len(alphas)
    one = jnp.ones((SUB, LANES), jnp.float32)
    term = [one] + [None] * (count - 1)
    real = [one] + [None] * (count - 1)
    imag = [None] * count
    for order in range(1, taylor_terms):
        fresh = []
        for i in range(count):
            pieces = []
            if term[i] is not None:
                pieces.append(alphas[i] * term[i])
            if i + 1 < count and term[i + 1] is not None:
                pieces.append(betas[i] * term[i + 1])
            if i > 0 and term[i - 1] is not None:
                pieces.append(betas[i - 1] * term[i - 1])
            fresh.append(sum(pieces[1:], pieces[0]) * (time_step / order) if pieces else None)
        term = fresh
        into = imag if order % 2 else real
        minus = order % 4 in (1, 2)
        for i in range(count):
            if term[i] is not None:
                if into[i] is None:
                    into[i] = -term[i] if minus else term[i]
                else:
                    into[i] = into[i] - term[i] if minus else into[i] + term[i]
    zero = jnp.zeros((SUB, LANES), jnp.float32)
    return [zero if r is None else r for r in real], [zero if m is None else m for m in imag]


def interleave(a, b, n):
    low = lax.broadcasted_iota(jnp.int32, (n, SUB, LANES), 1) < HALF
    return (jnp.where(low, a, pltpu.roll(b, HALF, 1)), jnp.where(low, pltpu.roll(a, HALF, 1), b))


def unpack_kernel(n, nx, back, out_hbm, out, sem):
    def put(x):
        return pltpu.make_async_copy(out.at[:, x], out_hbm.at[:, x], sem)

    for x in range(nx):
        for p, block in enumerate(interleave(back[0, :, x], back[1, :, x], n)):
            out[p, x] = block.reshape(n * SUB, LANES).T
        if x:
            put(x - 1).start()
    put(nx - 1).start()
    pltpu.make_async_copy(out, out_hbm, sem).wait()


def kernel(n, nx, nz, psi_hbm, pot_hbm, back, psi_ref, pot_ref, send, recv, extra, basis, inner, outb, outx, pots, mix,
           note, heard, send_sem, recv_sem, extra_send, extra_recv, pot_send, pot_recv, back_send, back_recv,
           far_send, note_send, note_recv, psi_sem, pot_sem, held):
    me = lax.axis_index("dom")
    mesh_ids = pl.DeviceIdType.MESH
    barrier = pltpu.get_barrier_semaphore()

    ratio = -0.5 * far_weight
    half = n // 2
    reach = ITERS - 1
    deep = half - reach
    side = me // half
    base = side * half
    opposite = half - base
    partner = lax.rem(me + half, n)
    near = half - side * reach
    outer = jnp.logical_or(me < deep, me >= n - deep)
    plane = n // 4
    spot = lax.rem(me, plane)
    inward = jnp.logical_and(me >= plane, me < n - plane)
    far_plane = (1 - side) * (n - plane)

    def greet(k, carry):
        pl.semaphore_signal(barrier, inc=1, device_id={"dom": lax.rem(me + k, n)}, device_id_type=mesh_ids)
        return carry

    lax.fori_loop(1, n, greet, 0)

    def take_psi(x):
        return pltpu.make_async_copy(psi_hbm.at[:, x], psi_ref.at[:, x], psi_sem.at[x])

    take_pot = pltpu.make_async_copy(pot_hbm, pot_ref, pot_sem)
    take_pot.start()
    for x in range(nx):
        take_psi(x).start()

    def remote(src, dst, send_to, recv_to, there):
        return pltpu.make_async_remote_copy(
            src_ref=src, dst_ref=dst, send_sem=send_to, recv_sem=recv_to,
            device_id={"dom": there}, device_id_type=mesh_ids)

    def forward(c, here, there):
        return remote(send.at[c, there], recv.at[c, here + 1], send_sem.at[c], recv_sem.at[c, here // plane], there)

    def beside(c, here, there):
        return remote(send.at[c, lax.rem(there + half, n)], extra.at[c, lax.rem(here, half) + 1],
                      extra_send.at[c], extra_recv.at[c], there)

    def pot_copy(here, there):
        return remote(pots.at[me], pots.at[here], pot_send, pot_recv, there)

    def backward(c, owner, there):
        return remote(outb.at[c, there], back.at[c, owner], back_send.at[c], back_recv.at[c], there)

    def far_copy(c, i, there):
        return remote(outx.at[c, i], back.at[c, partner], far_send.at[c], back_recv.at[c], there)

    def note_copy(c):
        return remote(note.at[c], heard.at[c], note_send.at[c], note_recv.at[c], partner)

    def pack(x, carry):
        take_psi(x).wait()
        parts = [psi_ref[p, x].T.reshape(n, SUB, LANES) for p in range(2)]
        for c, block in enumerate(interleave(*parts, n)):
            send[c, :, x] = block
        return carry

    lax.fori_loop(0, nx, pack, 0, unroll=4)

    take_pot.wait()
    pot_rows = jnp.concatenate([pot_ref[:, j, :] for j in range(LANES // nz)], axis=1)
    pots[me] = (pot_rows + -0.5 * centre_weight) * (1.0 / ratio)
    blank = jnp.zeros((nx, SUB, LANES), jnp.float32)
    for c in range(CHUNKS):
        recv[c, me + 1] = send[c, me]
        recv[c, 0] = blank
        recv[c, n + 1] = blank
        extra[c, me - base + 1] = send[c, partner]
        extra[c, 0] = blank
        extra[c, half + 1] = blank
    for j in range(ITERS - 1):
        basis[j, 0] = blank
        basis[j, n + 1] = blank
        inner[j, 0] = blank
        inner[j, half + 1] = blank

    pl.semaphore_wait(barrier, n - 1)

    def send_pot(k, carry):
        pot_copy(me, lax.rem(me + k, n)).start()
        return carry

    lax.fori_loop(1, n, send_pot, 0)

    def sends(c):
        def across(k, carry):
            there = far_plane + lax.rem(spot + k, plane)
            forward(c, me, there).start()
            return carry

        def across_near(k, carry):
            there = plane * (2 - side) + lax.rem(spot + k, plane)
            forward(c, me, there).start()
            return carry

        def home(k, carry):
            forward(c, me, base + lax.rem(me + k, half)).start()
            return carry

        def cross():
            lax.fori_loop(0, plane, across, 0)
            lax.fori_loop(0, plane, across_near, 0)

        def within():
            lax.fori_loop(1, half, home, 0)

        return cross, within

    def send_beside(c):
        def one(k, carry):
            beside(c, me, base + lax.rem(me + k, half)).start()
            return carry

        lax.fori_loop(1, half, one, 0)

    def landed(blocks, arrived):
        remote(blocks, blocks, note_send.at[0], arrived, partner).wait_recv()

    def left(blocks, departed):
        remote(blocks, blocks, departed, note_recv.at[0], partner).wait_send()

    def send_all(c):
        cross, within = sends(c)
        within()
        cross()

    upper = lax.broadcasted_iota(jnp.int32, (SUB, LANES), 1) >= nz
    lane = lax.broadcasted_iota(jnp.int32, (SUB, LANES), 1)
    sign = jnp.where(lax.broadcasted_iota(jnp.int32, (SUB, LANES), 0) < HALF, 1.0, -1.0)

    row = lax.broadcasted_iota(jnp.int32, (LANES, LANES), 0)
    column = lax.broadcasted_iota(jnp.int32, (LANES, LANES), 1)
    apart = lax.rem(row - column + 2 * nz, nz)
    near_z = jnp.where(jnp.logical_or(apart == 1, apart == nz - 1), 16.0, 0.0)
    far_z = jnp.where(jnp.logical_or(apart == 2, apart == nz - 2), 1.0, 0.0)
    same = (row < nz) == (column < nz)
    lanes_matrix = jnp.where(same, far_z - near_z, jnp.where(apart == 0, -16.0, 0.0)).astype(jnp.bfloat16)
    mix[0:LANES] = lanes_matrix
    mix[LANES:2 * LANES] = lanes_matrix

    def applied_at(ref, s, slab, size):
        slabs = [[ref[s + g, x] for x in range(nx)] for g in range(size + 2)]
        inside = jnp.concatenate([u for row_of in slabs[1:-1] for u in row_of], axis=0)
        high = inside.astype(jnp.bfloat16)
        rest = (inside - high.astype(jnp.float32)).astype(jnp.bfloat16)
        mixed = jnp.dot(jnp.concatenate([high, rest], axis=1), mix[...], preferred_element_type=jnp.float32)
        result = []
        for g in range(size):
            before, now, after = slabs[g:g + 3]
            for x in range(nx):
                u = now[x]
                close = now[(x + 1) % nx] + now[(x - 1) % nx]
                close = close + pltpu.roll(jnp.where(upper, before[x], after[x]), nz, 1)
                wide = now[(x + 2) % nx] + now[(x - 2) % nx] + before[x] + after[x]
                at = (g * nx + x) * SUB
                wide = wide + mixed[at:at + SUB]
                own = jnp.broadcast_to(pots[slab + g, pl.ds(x, 1), :], (SUB, LANES))
                result.append((own * u + (wide - 16.0 * close), u))
        return result

    def blend(us, straight, crossed):
        a = straight[0] * us[0]
        b = crossed[0] * us[0]
        for j in range(1, ITERS):
            a = a + straight[j] * us[j]
            b = b + crossed[j] * us[j]
        return a + swap_parts(b)

    send_all(0)

    @pl.when(inward)
    def _():
        landed(recv.at[0, pl.ds(0, plane)], recv_sem.at[0, far_plane // plane])

    send_all(1)
    send_beside(0)
    send_beside(1)

    def chunk(c, carry):
        vectors = [recv.at[c]] + [basis.at[j] for j in range(ITERS - 1)]

        own = me // plane * plane
        beyond = base + lax.rem(me - base + plane, half) // plane * plane
        across = plane * (2 - side)
        acc = jnp.zeros((SUB, LANES), jnp.float32)
        for first, count in ((own, plane - 1), (beyond, plane), (across, plane), (far_plane, plane)):
            blocks = recv.at[c, pl.ds(0, count)]
            arrived = recv_sem.at[c, first // plane]
            if first is far_plane:
                @pl.when(jnp.logical_not(jnp.logical_and(inward, c == 0)))
                def _(blocks=blocks, arrived=arrived):
                    landed(blocks, arrived)
            else:
                landed(blocks, arrived)

            def sum_up(k, acc, first=first):
                for x in range(nx):
                    u = recv[c, first + k + 1, x]
                    acc = acc + u * u
                return acc

            acc = lax.fori_loop(0, plane, sum_up, acc, unroll=True)
        square = total_of(acc) + epsilon
        scale = lax.rsqrt(square)
        first_norm = square * scale

        @pl.when(jnp.logical_and(c > 0, inward))
        def _():
            def kept(k, carry):
                backward(c - 1, me, near + lax.rem(me + k, reach)).start()
                return carry

            del kept

        @pl.when(c == 0)
        def _():
            landed(pots.at[pl.ds(0, n - 1)], pot_recv)

        scales, steps = [scale], []
        alphas, betas, selves, previous = [], [], [], []
        zero = jnp.zeros((SUB, LANES), jnp.float32)
        for j in range(ITERS):
            ref = vectors[j]
            products = [zero, zero]
            squares = [zero, zero]
            done = 0
            for g in range(n // GROUP + 1):
                if j and g < n // GROUP:
                    for s in range(g * GROUP, (g + 1) * GROUP):
                        for x in range(nx):
                            r = steps[-1] * held[(j - 1) % 2, s, x] - selves[-1] * vectors[j - 1][s + 1, x]
                            if j > 1:
                                r = r - previous[-1] * vectors[j - 2][s + 1, x]
                            ref[s + 1, x] = r
                            squares[x % 2] = squares[x % 2] + r * r
                if j and g == n // GROUP:
                    square = total_of(squares[0] + squares[1]) + epsilon
                upto = n if g == n // GROUP else (g + 1) * GROUP - 1
                for at, (w, u) in enumerate(applied_at(ref, done, done, upto - done)):
                    if j + 1 < ITERS:
                        held[j % 2, done + at // nx, at % nx] = w
                    products[at % 2] = products[at % 2] + u * w
                done = upto
            if j:
                scale = lax.rsqrt(square)
                scales.append(scale)
                betas.append(square * scale)
            step = scale * ratio
            alpha = step * (scale * total_of(products[0] + products[1]))
            alphas.append(alpha)
            if j + 1 < ITERS:
                steps.append(step)
                selves.append(alpha * scale)
                previous.append(betas[-1] * scales[-2] if j else None)

        real, imag = krylov_weights(alphas, betas)
        straight = [first_norm * scales[j] * real[j] for j in range(ITERS)]
        crossed = [first_norm * scales[j] * imag[j] * sign for j in range(ITERS)]

        told = zero
        for k, value in enumerate(steps + selves + previous[1:] + straight + crossed):
            told = jnp.where(lane == k, value, told)
        note[c] = told

        def combined(d, x):
            return blend([v[d + 1, x] for v in vectors], straight, crossed)

        def finish_across(k, carry):
            there = near + lax.rem(me + k, reach)
            for x in range(nx):
                outb[c, there, x] = combined(there, x)

            @pl.when(k == 0)
            def _():
                note_copy(c).start()

            @pl.when(jnp.logical_and(k == 1, jnp.logical_and(c > 0, inward)))
            def _():
                def late(i, carry):
                    backward(c - 1, me, near + lax.rem(me + i, reach)).start()
                    return carry

                lax.fori_loop(0, reach, late, 0)

            @pl.when(jnp.logical_and(k > 0, jnp.logical_or(c == CHUNKS - 1, jnp.logical_not(inward))))
            def _():
                backward(c, me, near + lax.rem(me + k - 1, reach)).start()

            return carry

        lax.fori_loop(0, reach, finish_across, 0)

        def finish_home(k, carry):
            there = base + lax.rem(me + k, half)
            for x in range(nx):
                outb[c, there, x] = combined(there, x)

            @pl.when(jnp.logical_and(k == 1, jnp.logical_or(c == CHUNKS - 1, jnp.logical_not(inward))))
            def _():
                backward(c, me, near + lax.rem(me + reach - 1, reach)).start()

            @pl.when(k > 1)
            def _():
                backward(c, me, base + lax.rem(me + k - 1, half)).start()

            return carry

        lax.fori_loop(1, half, finish_home, 0)
        for x in range(nx):
            back[c, me, x] = combined(me, x)
        backward(c, me, base + lax.rem(me + half - 1, half)).start()

        return carry

    def assist(c, carry):
        landed(extra.at[c, pl.ds(0, half - 1)], extra_recv.at[c])
        note_copy(c).wait_recv()
        words = heard[c]
        word = [jnp.broadcast_to(words[:, k:k + 1], (SUB, LANES)) for k in range(3 * reach - 1 + 2 * ITERS)]
        steps, selves, previous = word[:reach], word[reach:2 * reach], [None] + word[2 * reach:3 * reach - 1]
        straight, crossed = word[3 * reach - 1:3 * reach - 1 + ITERS], word[3 * reach - 1 + ITERS:]

        halves = [extra.at[c]] + [inner.at[j] for j in range(reach)]
        for j in range(reach):
            count = half - 1 - j
            start = (j + 1) * side
            pieces = -(-count // GROUP)
            at = 0
            for piece in range(pieces):
                size = (count - at) // (pieces - piece)
                for i, (w, u) in enumerate(applied_at(halves[j], start + at, base + start + at, size)):
                    here = start + at + i // nx + 1
                    r = steps[j] * w - selves[j] * u
                    if j:
                        r = r - previous[j] * halves[j - 1][here, i % nx]
                    halves[j + 1][here, i % nx] = r
                at += size

        first = reach * side
        for i in range(deep):
            for x in range(nx):
                outx[c, i, x] = blend([v[first + i + 1, x] for v in halves], straight, crossed)
        for i in range(deep):
            there = base + first + i

            @pl.when(there == me)
            def _(i=i):
                back[c, partner] = outx[c, i]

            @pl.when(there != me)
            def _(i=i, there=there):
                far_copy(c, i, there).start()

        return carry

    lax.fori_loop(0, CHUNKS, chunk, 0)
    lax.fori_loop(0, CHUNKS, assist, 0)

    left(pots.at[pl.ds(0, n - 1)], pot_send)
    for c in range(CHUNKS):
        left(send.at[c, pl.ds(0, n - 1)], send_sem.at[c])
        left(send.at[c, pl.ds(0, half - 1)], extra_send.at[c])
        note_copy(c).wait_send()

    for mine, count in ((outer, n - 2), (jnp.logical_not(outer), n - 1)):
        @pl.when(mine)
        def _(count=count):
            for c in range(CHUNKS):
                landed(back.at[c, pl.ds(0, count)], back_recv.at[c])
                left(outx.at[c, pl.ds(0, count - n + 1 + deep)], far_send.at[c])

    for c in range(CHUNKS):
        left(outb.at[c, pl.ds(0, reach + half - 1)], back_send.at[c])


def fused(psi, potential, n):
    parts, slabs, nx, by, nz, orbs = psi.shape
    half, reach = n // 2, ITERS - 1
    vec = lambda *lead: pltpu.VMEM(lead + (nx, SUB, LANES), jnp.float32)
    tile = lambda *lead: pltpu.VMEM(lead + (SUB, LANES), jnp.float32)
    dma = lambda *shape: pltpu.SemaphoreType.DMA(shape)
    result = pl.pallas_call(
        functools.partial(kernel, n, nx, nz),
        out_shape=pltpu.VMEM((CHUNKS, n, nx, SUB, LANES), jnp.float32),
        in_specs=[pl.BlockSpec(memory_space=pl.ANY)] * 2,
        out_specs=pl.BlockSpec(memory_space=pltpu.VMEM),
        scratch_shapes=[
            pltpu.VMEM((parts, nx, by * nz, orbs), jnp.float32), pltpu.VMEM((nx, by, nz), jnp.float32),
            vec(CHUNKS, n), vec(CHUNKS, n + 2), vec(CHUNKS, half + 2), vec(reach, n + 2), vec(reach, half + 2),
            vec(CHUNKS, n), vec(CHUNKS, half - reach),
            pltpu.VMEM((n, nx, LANES), jnp.float32), pltpu.VMEM((2 * LANES, LANES), jnp.bfloat16),
            tile(CHUNKS), tile(CHUNKS),
            dma(CHUNKS), dma(CHUNKS, 4), dma(CHUNKS), dma(CHUNKS), dma(), dma(),
            dma(CHUNKS), dma(CHUNKS), dma(CHUNKS), dma(CHUNKS), dma(CHUNKS), dma(nx), dma(), vec(2, n),
        ],
        compiler_params=pltpu.CompilerParams(collective_id=0, has_side_effects=True),
    )(psi.reshape(parts, nx, by * nz, orbs), potential.reshape(nx, by, nz))
    out = pl.pallas_call(
        functools.partial(unpack_kernel, n, nx),
        out_shape=jax.ShapeDtypeStruct((parts, nx, by * nz, orbs), jnp.float32),
        in_specs=[pl.BlockSpec(memory_space=pltpu.VMEM)],
        out_specs=pl.BlockSpec(memory_space=pl.ANY),
        scratch_shapes=[pltpu.VMEM((parts, nx, by * nz, orbs), jnp.float32), dma()],
    )(pltpu.with_memory_space_constraint(result, pltpu.VMEM))
    return out.reshape(psi.shape)


def fits(psi, n):
    parts, slabs, nx, by, nz, orbs = psi.shape
    return parts == 2 and slabs == 1 and by == 2 and by * nz == LANES and orbs == LANES and orbs == n * SUB and n % GROUP == 0 and n // 2 > ITERS


def per_device(n, psi, potential):
    if fits(psi, n):
        return fused(psi, potential, n)
    return on_device(psi, potential)


def solution(mesh):
    placed = (P(None, "dom", None, None, None, "st"), P("dom", None, None, None))
    return jax.shard_map(
        functools.partial(per_device, mesh.shape["dom"]),
        mesh=mesh,
        in_specs=placed,
        out_specs=P(None, "dom", None, None, None, "st"),
        check_vma=False,
    )
```

```python
import functools

import jax
import jax.numpy as jnp
from jax import lax
from jax.experimental import pallas as pl
from jax.experimental.pallas import tpu as pltpu
from jax.sharding import PartitionSpec as P

ITERS = 6


epsilon = 1e-06
time_step = 0.5
taylor_terms = 32
far_weight = -1.0 / 12.0
near_weight = 4.0 / 3.0
centre_weight = -7.5


def to_grid(blocked):
    parts, nblocks, cx, by, nz, orbs = blocked.shape
    grid = blocked.transpose(0, 2, 1, 3, 4, 5)
    return grid.reshape(parts, cx, nblocks * by, nz, orbs)


def to_blocks(grid, by):
    parts, nx, ny, nz, orbs = grid.shape
    blocked = grid.reshape(parts, nx, ny // by, by, nz, orbs).transpose(0, 2, 1, 3, 4, 5)
    return blocked


def shift_walls(values, offset):
    width_y = values.shape[2]
    padded = jnp.pad(values, ((0, 0), (0, 0), (2, 2), (0, 0), (0, 0)))
    return padded[:, :, 2 - offset : 2 - offset + width_y]


def hamiltonian_whole(values_in, potential):
    total = centre_weight * values_in
    for along in (1, 3):
        total = total + near_weight * (
            jnp.roll(values_in, 1, along) + jnp.roll(values_in, -1, along)
        )
        total = total + far_weight * (
            jnp.roll(values_in, 2, along) + jnp.roll(values_in, -2, along)
        )
    total = total + near_weight * (shift_walls(values_in, 1) + shift_walls(values_in, -1))
    total = total + far_weight * (shift_walls(values_in, 2) + shift_walls(values_in, -2))
    return -0.5 * total + potential[None, :, :, :, None] * values_in


def tridiagonal(alphas, betas, vector):
    zero_row = jnp.zeros((1, vector.shape[1]), jnp.float32)
    upper = jnp.concatenate([betas * vector[1:], zero_row], axis=0)
    lower = jnp.concatenate([zero_row, betas * vector[:-1]], axis=0)
    return alphas * vector + upper + lower


def krylov_exponential(alphas, betas):
    count = alphas.shape[0]
    first = (jnp.arange(count) == 0).astype(jnp.float32)[:, None] * jnp.ones_like(alphas)
    term_real = first
    term_imag = jnp.zeros_like(alphas)
    sum_real = term_real
    sum_imag = term_imag
    for order in range(1, taylor_terms):
        applied_real = tridiagonal(alphas, betas, term_real)
        applied_imag = tridiagonal(alphas, betas, term_imag)
        term_real = time_step * applied_imag / order
        term_imag = -time_step * applied_real / order
        sum_real = sum_real + term_real
        sum_imag = sum_imag + term_imag
    return (sum_real, sum_imag)


def combine_basis(krylov_basis, alpha_list, beta_list, first_norm):
    coef_real, coef_imag = krylov_exponential(jnp.stack(alpha_list), jnp.stack(beta_list))
    out_real = jnp.zeros_like(krylov_basis[0][0])
    out_imag = jnp.zeros_like(krylov_basis[0][0])
    for index_j in range(len(krylov_basis)):
        basis_now = krylov_basis[index_j]
        out_real = out_real + coef_real[index_j] * basis_now[0] - coef_imag[index_j] * basis_now[1]
        out_imag = out_imag + coef_real[index_j] * basis_now[1] + coef_imag[index_j] * basis_now[0]
    return first_norm * jnp.stack([out_real, out_imag])


def local_lanczos(grid_psi, grid_pot):
    axes_all = (0, 1, 2, 3)
    first_norm = jnp.sqrt(jnp.sum(grid_psi * grid_psi, axis=axes_all) + epsilon)
    vector = grid_psi / first_norm
    previous = jnp.zeros_like(vector)
    beta_prev = jnp.zeros_like(first_norm)
    krylov_basis = []
    alpha_list = []
    beta_list = []
    for iteration in range(ITERS):
        applied = hamiltonian_whole(vector, grid_pot)
        alpha_now = jnp.sum(vector * applied, axis=axes_all)
        krylov_basis.append(vector)
        alpha_list.append(alpha_now)
        if iteration + 1 < ITERS:
            remainder = applied - alpha_now * vector - beta_prev * previous
            beta_now = jnp.sqrt(jnp.sum(remainder * remainder, axis=axes_all) + epsilon)
            previous = vector
            vector = remainder / beta_now
            beta_prev = beta_now
            beta_list.append(beta_now)
    return combine_basis(krylov_basis, alpha_list, beta_list, first_norm)


def on_device(psi, potential):
    by = psi.shape[3]
    moved = lax.all_to_all(psi, "dom", split_axis=5, concat_axis=1, tiled=True)
    whole_pot = lax.all_gather(potential, "dom", axis=0, tiled=True)
    grid_pot = to_grid(whole_pot[None, :, :, :, :, None])[0, :, :, :, 0]
    result = to_blocks(local_lanczos(to_grid(moved), grid_pot), by)
    return lax.all_to_all(result, "dom", split_axis=1, concat_axis=5, tiled=True)


SUB = 8
LANES = 128
HALF = SUB // 2
CHUNKS = 2
GROUP = 4


def swap_parts(x):
    return pltpu.roll(x, HALF, 0)


def total_of(acc):
    summed = jnp.broadcast_to(jnp.sum(acc, axis=1, keepdims=True), (SUB, LANES))
    return summed + swap_parts(summed)


def krylov_weights(alphas, betas):
    count = len(alphas)
    one = jnp.ones((SUB, LANES), jnp.float32)
    term = [one] + [None] * (count - 1)
    real = [one] + [None] * (count - 1)
    imag = [None] * count
    for order in range(1, taylor_terms):
        fresh = []
        for i in range(count):
            pieces = []
            if term[i] is not None:
                pieces.append(alphas[i] * term[i])
            if i + 1 < count and term[i + 1] is not None:
                pieces.append(betas[i] * term[i + 1])
            if i > 0 and term[i - 1] is not None:
                pieces.append(betas[i - 1] * term[i - 1])
            fresh.append(sum(pieces[1:], pieces[0]) * (time_step / order) if pieces else None)
        term = fresh
        into = imag if order % 2 else real
        minus = order % 4 in (1, 2)
        for i in range(count):
            if term[i] is not None:
                if into[i] is None:
                    into[i] = -term[i] if minus else term[i]
                else:
                    into[i] = into[i] - term[i] if minus else into[i] + term[i]
    zero = jnp.zeros((SUB, LANES), jnp.float32)
    return [zero if r is None else r for r in real], [zero if m is None else m for m in imag]


def interleave(a, b, n):
    low = lax.broadcasted_iota(jnp.int32, (n, SUB, LANES), 1) < HALF
    return (jnp.where(low, a, pltpu.roll(b, HALF, 1)), jnp.where(low, pltpu.roll(a, HALF, 1), b))


def unpack_kernel(n, nx, back, out_hbm, out, sem):
    def put(x):
        return pltpu.make_async_copy(out.at[:, x], out_hbm.at[:, x], sem)

    for x in range(nx):
        for p, block in enumerate(interleave(back[0, :, x], back[1, :, x], n)):
            out[p, x] = block.reshape(n * SUB, LANES).T
        if x:
            put(x - 1).start()
    put(nx - 1).start()
    pltpu.make_async_copy(out, out_hbm, sem).wait()


def kernel(n, nx, nz, psi_hbm, pot_hbm, back, psi_ref, pot_ref, send, recv, extra, basis, inner, outb, outx, pots, mix,
           note, heard, send_sem, recv_sem, extra_send, extra_recv, pot_send, pot_recv, back_send, back_recv,
           far_send, note_send, note_recv, psi_sem, pot_sem, held):
    me = lax.axis_index("dom")
    mesh_ids = pl.DeviceIdType.MESH
    barrier = pltpu.get_barrier_semaphore()

    ratio = -0.5 * far_weight
    half = n // 2
    reach = ITERS - 1
    deep = half - reach
    side = me // half
    base = side * half
    opposite = half - base
    partner = lax.rem(me + half, n)
    near = half - side * reach
    outer = jnp.logical_or(me < deep, me >= n - deep)
    plane = n // 4
    spot = lax.rem(me, plane)
    inward = jnp.logical_and(me >= plane, me < n - plane)
    far_plane = (1 - side) * (n - plane)
    outward = jnp.logical_not(inward)

    def greet(k, carry):
        pl.semaphore_signal(barrier, inc=1, device_id={"dom": lax.rem(me + k, n)}, device_id_type=mesh_ids)
        return carry

    lax.fori_loop(1, n, greet, 0)

    def take_psi(x):
        return pltpu.make_async_copy(psi_hbm.at[:, x], psi_ref.at[:, x], psi_sem.at[x])

    take_pot = pltpu.make_async_copy(pot_hbm, pot_ref, pot_sem)
    take_pot.start()
    for x in range(nx):
        take_psi(x).start()

    def remote(src, dst, send_to, recv_to, there):
        return pltpu.make_async_remote_copy(
            src_ref=src, dst_ref=dst, send_sem=send_to, recv_sem=recv_to,
            device_id={"dom": there}, device_id_type=mesh_ids)

    def forward(c, here, there):
        return remote(send.at[c, there], recv.at[c, here + 1], send_sem.at[c], recv_sem.at[c, here // plane], there)

    def beside(c, here, there):
        return remote(send.at[c, lax.rem(there + half, n)], extra.at[c, lax.rem(here, half) + 1],
                      extra_send.at[c], extra_recv.at[c], there)

    def pot_copy(here, there):
        return remote(pots.at[me], pots.at[here], pot_send, pot_recv, there)

    def backward(c, owner, there):
        return remote(outb.at[c, there], back.at[c, owner], back_send.at[c], back_recv.at[c], there)

    def far_copy(c, i, there):
        return remote(outx.at[c, i], back.at[c, partner], far_send.at[c], back_recv.at[c], there)

    def note_copy(c):
        return remote(note.at[c], heard.at[c], note_send.at[c], note_recv.at[c], partner)

    def pack(x, carry):
        take_psi(x).wait()
        parts = [psi_ref[p, x].T.reshape(n, SUB, LANES) for p in range(2)]
        for c, block in enumerate(interleave(*parts, n)):
            send[c, :, x] = block
        return carry

    lax.fori_loop(0, nx, pack, 0, unroll=4)

    take_pot.wait()
    pot_rows = jnp.concatenate([pot_ref[:, j, :] for j in range(LANES // nz)], axis=1)
    pots[me] = (pot_rows + -0.5 * centre_weight) * (1.0 / ratio)
    blank = jnp.zeros((nx, SUB, LANES), jnp.float32)
    for c in range(CHUNKS):
        recv[c, me + 1] = send[c, me]
        recv[c, 0] = blank
        recv[c, n + 1] = blank
        extra[c, me - base + 1] = send[c, partner]
        extra[c, 0] = blank
        extra[c, half + 1] = blank
    for j in range(ITERS - 1):
        basis[j, 0] = blank
        basis[j, n + 1] = blank
        inner[j, 0] = blank
        inner[j, half + 1] = blank

    pl.semaphore_wait(barrier, n - 1)

    def send_pot(k, carry):
        pot_copy(me, lax.rem(me + k, n)).start()
        return carry

    lax.fori_loop(1, n, send_pot, 0)

    def send_far(c):
        def one(k, carry):
            forward(c, me, far_plane + lax.rem(spot + k, plane)).start()
            return carry

        lax.fori_loop(0, plane, one, 0)

    def send_near(c):
        def one(k, carry):
            forward(c, me, plane * (2 - side) + lax.rem(spot + k, plane)).start()
            return carry

        lax.fori_loop(0, plane, one, 0)

    def send_plane(c):
        def one(k, carry):
            forward(c, me, me - spot + lax.rem(spot + k, plane)).start()
            return carry

        lax.fori_loop(1, plane, one, 0)

    def send_next(c):
        def one(k, carry):
            forward(c, me, base + lax.rem(me - spot - base + plane, half) + lax.rem(spot + k, plane)).start()
            return carry

        lax.fori_loop(0, plane, one, 0)

    def send_beside(c):
        def one(k, carry):
            beside(c, me, base + lax.rem(me + k, half)).start()
            return carry

        lax.fori_loop(1, half, one, 0)

    def landed(blocks, arrived):
        remote(blocks, blocks, note_send.at[0], arrived, partner).wait_recv()

    def left(blocks, departed):
        remote(blocks, blocks, departed, note_recv.at[0], partner).wait_send()

    upper = lax.broadcasted_iota(jnp.int32, (SUB, LANES), 1) >= nz
    lane = lax.broadcasted_iota(jnp.int32, (SUB, LANES), 1)
    sign = jnp.where(lax.broadcasted_iota(jnp.int32, (SUB, LANES), 0) < HALF, 1.0, -1.0)

    row = lax.broadcasted_iota(jnp.int32, (LANES, LANES), 0)
    column = lax.broadcasted_iota(jnp.int32, (LANES, LANES), 1)
    apart = lax.rem(row - column + 2 * nz, nz)
    near_z = jnp.where(jnp.logical_or(apart == 1, apart == nz - 1), 16.0, 0.0)
    far_z = jnp.where(jnp.logical_or(apart == 2, apart == nz - 2), 1.0, 0.0)
    same = (row < nz) == (column < nz)
    lanes_matrix = jnp.where(same, far_z - near_z, jnp.where(apart == 0, -16.0, 0.0)).astype(jnp.bfloat16)
    mix[0:LANES] = lanes_matrix
    mix[LANES:2 * LANES] = lanes_matrix

    def applied_at(ref, s, slab, size):
        slabs = [[ref[s + g, x] for x in range(nx)] for g in range(size + 2)]
        inside = jnp.concatenate([u for row_of in slabs[1:-1] for u in row_of], axis=0)
        high = inside.astype(jnp.bfloat16)
        rest = (inside - high.astype(jnp.float32)).astype(jnp.bfloat16)
        mixed = jnp.dot(jnp.concatenate([high, rest], axis=1), mix[...], preferred_element_type=jnp.float32)
        result = []
        for g in range(size):
            before, now, after = slabs[g:g + 3]
            for x in range(nx):
                u = now[x]
                close = now[(x + 1) % nx] + now[(x - 1) % nx]
                close = close + pltpu.roll(jnp.where(upper, before[x], after[x]), nz, 1)
                wide = now[(x + 2) % nx] + now[(x - 2) % nx] + before[x] + after[x]
                at = (g * nx + x) * SUB
                wide = wide + mixed[at:at + SUB]
                own = jnp.broadcast_to(pots[slab + g, pl.ds(x, 1), :], (SUB, LANES))
                result.append((own * u + (wide - 16.0 * close), u))
        return result

    def blend(us, straight, crossed):
        a = straight[0] * us[0]
        b = crossed[0] * us[0]
        for j in range(1, ITERS):
            a = a + straight[j] * us[j]
            b = b + crossed[j] * us[j]
        return a + swap_parts(b)

    @pl.when(outward)
    def _():
        send_next(0)
        send_plane(0)
        send_far(0)
        send_near(0)
        send_next(1)
        send_plane(1)
        send_far(1)
        send_near(1)
        send_beside(0)
        send_beside(1)

    @pl.when(inward)
    def _():
        send_plane(0)
        send_near(0)
        send_far(0)
        send_next(0)
        send_next(1)
        send_plane(1)
        send_beside(0)
        send_beside(1)
        landed(recv.at[0, pl.ds(0, plane)], recv_sem.at[0, far_plane // plane])
        send_near(1)
        send_far(1)

    def chunk(c, carry):
        vectors = [recv.at[c]] + [basis.at[j] for j in range(ITERS - 1)]

        own = me // plane * plane
        beyond = base + lax.rem(me - base + plane, half) // plane * plane
        across = plane * (2 - side)
        acc = jnp.zeros((SUB, LANES), jnp.float32)
        for first, count in ((own, plane - 1), (beyond, plane), (across, plane), (far_plane, plane)):
            blocks = recv.at[c, pl.ds(0, count)]
            arrived = recv_sem.at[c, first // plane]
            if first is far_plane:
                @pl.when(jnp.logical_not(jnp.logical_and(inward, c == 0)))
                def _(blocks=blocks, arrived=arrived):
                    landed(blocks, arrived)
            else:
                landed(blocks, arrived)

            def sum_up(k, acc, first=first):
                for x in range(nx):
                    u = recv[c, first + k + 1, x]
                    acc = acc + u * u
                return acc

            acc = lax.fori_loop(0, plane, sum_up, acc, unroll=True)
        square = total_of(acc) + epsilon
        scale = lax.rsqrt(square)
        first_norm = square * scale

        @pl.when(c == 0)
        def _():
            landed(pots.at[pl.ds(0, n - 1)], pot_recv)

        scales, steps = [scale], []
        alphas, betas, selves, previous = [], [], [], []
        zero = jnp.zeros((SUB, LANES), jnp.float32)
        for j in range(ITERS):
            ref = vectors[j]
            products = [zero, zero]
            squares = [zero, zero]
            done = 0
            for g in range(n // GROUP + 1):
                if j and g < n // GROUP:
                    for s in range(g * GROUP, (g + 1) * GROUP):
                        for x in range(nx):
                            r = steps[-1] * held[(j - 1) % 2, s, x] - selves[-1] * vectors[j - 1][s + 1, x]
                            if j > 1:
                                r = r - previous[-1] * vectors[j - 2][s + 1, x]
                            ref[s + 1, x] = r
                            squares[x % 2] = squares[x % 2] + r * r
                if j and g == n // GROUP:
                    square = total_of(squares[0] + squares[1]) + epsilon
                upto = n if g == n // GROUP else (g + 1) * GROUP - 1
                for at, (w, u) in enumerate(applied_at(ref, done, done, upto - done)):
                    if j + 1 < ITERS:
                        held[j % 2, done + at // nx, at % nx] = w
                    products[at % 2] = products[at % 2] + u * w
                done = upto
            if j:
                scale = lax.rsqrt(square)
                scales.append(scale)
                betas.append(square * scale)
            step = scale * ratio
            alpha = step * (scale * total_of(products[0] + products[1]))
            alphas.append(alpha)
            if j + 1 < ITERS:
                steps.append(step)
                selves.append(alpha * scale)
                previous.append(betas[-1] * scales[-2] if j else None)

        real, imag = krylov_weights(alphas, betas)
        straight = [first_norm * scales[j] * real[j] for j in range(ITERS)]
        crossed = [first_norm * scales[j] * imag[j] * sign for j in range(ITERS)]

        told = zero
        for k, value in enumerate(steps + selves + previous[1:] + straight + crossed):
            told = jnp.where(lane == k, value, told)
        note[c] = told

        def combined(d, x):
            return blend([v[d + 1, x] for v in vectors], straight, crossed)

        def finish_across(k, carry):
            there = near + lax.rem(me + k, reach)
            for x in range(nx):
                outb[c, there, x] = combined(there, x)

            @pl.when(k == 0)
            def _():
                note_copy(c).start()

            @pl.when(jnp.logical_and(k == 1, jnp.logical_and(c > 0, inward)))
            def _():
                def late(i, carry):
                    backward(c - 1, me, near + lax.rem(me + i, reach)).start()
                    return carry

                lax.fori_loop(0, reach, late, 0)

            @pl.when(jnp.logical_and(k > 0, jnp.logical_or(c == CHUNKS - 1, jnp.logical_not(inward))))
            def _():
                backward(c, me, near + lax.rem(me + k - 1, reach)).start()

            return carry

        lax.fori_loop(0, reach, finish_across, 0)

        def finish_home(k, carry):
            there = base + lax.rem(me + k, half)
            for x in range(nx):
                outb[c, there, x] = combined(there, x)

            @pl.when(jnp.logical_and(k == 1, jnp.logical_or(c == CHUNKS - 1, jnp.logical_not(inward))))
            def _():
                backward(c, me, near + lax.rem(me + reach - 1, reach)).start()

            @pl.when(k > 1)
            def _():
                backward(c, me, base + lax.rem(me + k - 1, half)).start()

            return carry

        lax.fori_loop(1, half, finish_home, 0)
        for x in range(nx):
            back[c, me, x] = combined(me, x)
        backward(c, me, base + lax.rem(me + half - 1, half)).start()

        return carry

    def assist(c, carry):
        landed(extra.at[c, pl.ds(0, half - 1)], extra_recv.at[c])
        note_copy(c).wait_recv()
        words = heard[c]
        word = [jnp.broadcast_to(words[:, k:k + 1], (SUB, LANES)) for k in range(3 * reach - 1 + 2 * ITERS)]
        steps, selves, previous = word[:reach], word[reach:2 * reach], [None] + word[2 * reach:3 * reach - 1]
        straight, crossed = word[3 * reach - 1:3 * reach - 1 + ITERS], word[3 * reach - 1 + ITERS:]

        halves = [extra.at[c]] + [inner.at[j] for j in range(reach)]
        for j in range(reach):
            count = half - 1 - j
            start = (j + 1) * side
            pieces = -(-count // GROUP)
            at = 0
            for piece in range(pieces):
                size = (count - at) // (pieces - piece)
                for i, (w, u) in enumerate(applied_at(halves[j], start + at, base + start + at, size)):
                    here = start + at + i // nx + 1
                    r = steps[j] * w - selves[j] * u
                    if j:
                        r = r - previous[j] * halves[j - 1][here, i % nx]
                    halves[j + 1][here, i % nx] = r
                at += size

        first = reach * side
        for i in range(deep):
            for x in range(nx):
                outx[c, i, x] = blend([v[first + i + 1, x] for v in halves], straight, crossed)
        for i in range(deep):
            there = base + first + i

            @pl.when(there == me)
            def _(i=i):
                back[c, partner] = outx[c, i]

            @pl.when(there != me)
            def _(i=i, there=there):
                far_copy(c, i, there).start()

        return carry

    lax.fori_loop(0, CHUNKS, chunk, 0)
    lax.fori_loop(0, CHUNKS, assist, 0)

    left(pots.at[pl.ds(0, n - 1)], pot_send)
    for c in range(CHUNKS):
        left(send.at[c, pl.ds(0, n - 1)], send_sem.at[c])
        left(send.at[c, pl.ds(0, half - 1)], extra_send.at[c])
        note_copy(c).wait_send()

    for mine, count in ((outer, n - 2), (jnp.logical_not(outer), n - 1)):
        @pl.when(mine)
        def _(count=count):
            for c in range(CHUNKS):
                landed(back.at[c, pl.ds(0, count)], back_recv.at[c])
                left(outx.at[c, pl.ds(0, count - n + 1 + deep)], far_send.at[c])

    for c in range(CHUNKS):
        left(outb.at[c, pl.ds(0, reach + half - 1)], back_send.at[c])


def fused(psi, potential, n):
    parts, slabs, nx, by, nz, orbs = psi.shape
    half, reach = n // 2, ITERS - 1
    vec = lambda *lead: pltpu.VMEM(lead + (nx, SUB, LANES), jnp.float32)
    tile = lambda *lead: pltpu.VMEM(lead + (SUB, LANES), jnp.float32)
    dma = lambda *shape: pltpu.SemaphoreType.DMA(shape)
    result = pl.pallas_call(
        functools.partial(kernel, n, nx, nz),
        out_shape=pltpu.VMEM((CHUNKS, n, nx, SUB, LANES), jnp.float32),
        in_specs=[pl.BlockSpec(memory_space=pl.ANY)] * 2,
        out_specs=pl.BlockSpec(memory_space=pltpu.VMEM),
        scratch_shapes=[
            pltpu.VMEM((parts, nx, by * nz, orbs), jnp.float32), pltpu.VMEM((nx, by, nz), jnp.float32),
            vec(CHUNKS, n), vec(CHUNKS, n + 2), vec(CHUNKS, half + 2), vec(reach, n + 2), vec(reach, half + 2),
            vec(CHUNKS, n), vec(CHUNKS, half - reach),
            pltpu.VMEM((n, nx, LANES), jnp.float32), pltpu.VMEM((2 * LANES, LANES), jnp.bfloat16),
            tile(CHUNKS), tile(CHUNKS),
            dma(CHUNKS), dma(CHUNKS, 4), dma(CHUNKS), dma(CHUNKS), dma(), dma(),
            dma(CHUNKS), dma(CHUNKS), dma(CHUNKS), dma(CHUNKS), dma(CHUNKS), dma(nx), dma(), vec(2, n),
        ],
        compiler_params=pltpu.CompilerParams(collective_id=0, has_side_effects=True),
    )(psi.reshape(parts, nx, by * nz, orbs), potential.reshape(nx, by, nz))
    out = pl.pallas_call(
        functools.partial(unpack_kernel, n, nx),
        out_shape=jax.ShapeDtypeStruct((parts, nx, by * nz, orbs), jnp.float32),
        in_specs=[pl.BlockSpec(memory_space=pltpu.VMEM)],
        out_specs=pl.BlockSpec(memory_space=pl.ANY),
        scratch_shapes=[pltpu.VMEM((parts, nx, by * nz, orbs), jnp.float32), dma()],
    )(pltpu.with_memory_space_constraint(result, pltpu.VMEM))
    return out.reshape(psi.shape)


def fits(psi, n):
    parts, slabs, nx, by, nz, orbs = psi.shape
    return parts == 2 and slabs == 1 and by == 2 and by * nz == LANES and orbs == LANES and orbs == n * SUB and n % GROUP == 0 and n // 2 > ITERS


def per_device(n, psi, potential):
    if fits(psi, n):
        return fused(psi, potential, n)
    return on_device(psi, potential)


def solution(mesh):
    placed = (P(None, "dom", None, None, None, "st"), P("dom", None, None, None))
    return jax.shard_map(
        functools.partial(per_device, mesh.shape["dom"]),
        mesh=mesh,
        in_specs=placed,
        out_specs=P(None, "dom", None, None, None, "st"),
        check_vma=False,
    )
```

```python
import functools

import jax
import jax.numpy as jnp
from jax import lax
from jax.experimental import pallas as pl
from jax.experimental.pallas import tpu as pltpu
from jax.sharding import PartitionSpec as P

ITERS = 6


epsilon = 1e-06
time_step = 0.5
taylor_terms = 32
far_weight = -1.0 / 12.0
near_weight = 4.0 / 3.0
centre_weight = -7.5


def to_grid(blocked):
    parts, nblocks, cx, by, nz, orbs = blocked.shape
    grid = blocked.transpose(0, 2, 1, 3, 4, 5)
    return grid.reshape(parts, cx, nblocks * by, nz, orbs)


def to_blocks(grid, by):
    parts, nx, ny, nz, orbs = grid.shape
    blocked = grid.reshape(parts, nx, ny // by, by, nz, orbs).transpose(0, 2, 1, 3, 4, 5)
    return blocked


def shift_walls(values, offset):
    width_y = values.shape[2]
    padded = jnp.pad(values, ((0, 0), (0, 0), (2, 2), (0, 0), (0, 0)))
    return padded[:, :, 2 - offset : 2 - offset + width_y]


def hamiltonian_whole(values_in, potential):
    total = centre_weight * values_in
    for along in (1, 3):
        total = total + near_weight * (
            jnp.roll(values_in, 1, along) + jnp.roll(values_in, -1, along)
        )
        total = total + far_weight * (
            jnp.roll(values_in, 2, along) + jnp.roll(values_in, -2, along)
        )
    total = total + near_weight * (shift_walls(values_in, 1) + shift_walls(values_in, -1))
    total = total + far_weight * (shift_walls(values_in, 2) + shift_walls(values_in, -2))
    return -0.5 * total + potential[None, :, :, :, None] * values_in


def tridiagonal(alphas, betas, vector):
    zero_row = jnp.zeros((1, vector.shape[1]), jnp.float32)
    upper = jnp.concatenate([betas * vector[1:], zero_row], axis=0)
    lower = jnp.concatenate([zero_row, betas * vector[:-1]], axis=0)
    return alphas * vector + upper + lower


def krylov_exponential(alphas, betas):
    count = alphas.shape[0]
    first = (jnp.arange(count) == 0).astype(jnp.float32)[:, None] * jnp.ones_like(alphas)
    term_real = first
    term_imag = jnp.zeros_like(alphas)
    sum_real = term_real
    sum_imag = term_imag
    for order in range(1, taylor_terms):
        applied_real = tridiagonal(alphas, betas, term_real)
        applied_imag = tridiagonal(alphas, betas, term_imag)
        term_real = time_step * applied_imag / order
        term_imag = -time_step * applied_real / order
        sum_real = sum_real + term_real
        sum_imag = sum_imag + term_imag
    return (sum_real, sum_imag)


def combine_basis(krylov_basis, alpha_list, beta_list, first_norm):
    coef_real, coef_imag = krylov_exponential(jnp.stack(alpha_list), jnp.stack(beta_list))
    out_real = jnp.zeros_like(krylov_basis[0][0])
    out_imag = jnp.zeros_like(krylov_basis[0][0])
    for index_j in range(len(krylov_basis)):
        basis_now = krylov_basis[index_j]
        out_real = out_real + coef_real[index_j] * basis_now[0] - coef_imag[index_j] * basis_now[1]
        out_imag = out_imag + coef_real[index_j] * basis_now[1] + coef_imag[index_j] * basis_now[0]
    return first_norm * jnp.stack([out_real, out_imag])


def local_lanczos(grid_psi, grid_pot):
    axes_all = (0, 1, 2, 3)
    first_norm = jnp.sqrt(jnp.sum(grid_psi * grid_psi, axis=axes_all) + epsilon)
    vector = grid_psi / first_norm
    previous = jnp.zeros_like(vector)
    beta_prev = jnp.zeros_like(first_norm)
    krylov_basis = []
    alpha_list = []
    beta_list = []
    for iteration in range(ITERS):
        applied = hamiltonian_whole(vector, grid_pot)
        alpha_now = jnp.sum(vector * applied, axis=axes_all)
        krylov_basis.append(vector)
        alpha_list.append(alpha_now)
        if iteration + 1 < ITERS:
            remainder = applied - alpha_now * vector - beta_prev * previous
            beta_now = jnp.sqrt(jnp.sum(remainder * remainder, axis=axes_all) + epsilon)
            previous = vector
            vector = remainder / beta_now
            beta_prev = beta_now
            beta_list.append(beta_now)
    return combine_basis(krylov_basis, alpha_list, beta_list, first_norm)


def on_device(psi, potential):
    by = psi.shape[3]
    moved = lax.all_to_all(psi, "dom", split_axis=5, concat_axis=1, tiled=True)
    whole_pot = lax.all_gather(potential, "dom", axis=0, tiled=True)
    grid_pot = to_grid(whole_pot[None, :, :, :, :, None])[0, :, :, :, 0]
    result = to_blocks(local_lanczos(to_grid(moved), grid_pot), by)
    return lax.all_to_all(result, "dom", split_axis=1, concat_axis=5, tiled=True)


SUB = 8
LANES = 128
HALF = SUB // 2
CHUNKS = 2
GROUP = 4


def swap_parts(x):
    return pltpu.roll(x, HALF, 0)


def total_of(acc):
    summed = jnp.broadcast_to(jnp.sum(acc, axis=1, keepdims=True), (SUB, LANES))
    return summed + swap_parts(summed)


def krylov_weights(alphas, betas):
    count = len(alphas)
    one = jnp.ones((SUB, LANES), jnp.float32)
    term = [one] + [None] * (count - 1)
    real = [one] + [None] * (count - 1)
    imag = [None] * count
    for order in range(1, taylor_terms):
        fresh = []
        for i in range(count):
            pieces = []
            if term[i] is not None:
                pieces.append(alphas[i] * term[i])
            if i + 1 < count and term[i + 1] is not None:
                pieces.append(betas[i] * term[i + 1])
            if i > 0 and term[i - 1] is not None:
                pieces.append(betas[i - 1] * term[i - 1])
            fresh.append(sum(pieces[1:], pieces[0]) * (time_step / order) if pieces else None)
        term = fresh
        into = imag if order % 2 else real
        minus = order % 4 in (1, 2)
        for i in range(count):
            if term[i] is not None:
                if into[i] is None:
                    into[i] = -term[i] if minus else term[i]
                else:
                    into[i] = into[i] - term[i] if minus else into[i] + term[i]
    zero = jnp.zeros((SUB, LANES), jnp.float32)
    return [zero if r is None else r for r in real], [zero if m is None else m for m in imag]


def interleave(a, b, n):
    low = lax.broadcasted_iota(jnp.int32, (n, SUB, LANES), 1) < HALF
    return (jnp.where(low, a, pltpu.roll(b, HALF, 1)), jnp.where(low, pltpu.roll(a, HALF, 1), b))


def unpack_kernel(n, nx, back, out_hbm, out, sem):
    def put(x):
        return pltpu.make_async_copy(out.at[:, x], out_hbm.at[:, x], sem)

    for x in range(nx):
        for p, block in enumerate(interleave(back[0, :, x], back[1, :, x], n)):
            out[p, x] = block.reshape(n * SUB, LANES).T
        if x:
            put(x - 1).start()
    put(nx - 1).start()
    pltpu.make_async_copy(out, out_hbm, sem).wait()


def kernel(n, nx, nz, psi_hbm, pot_hbm, back, psi_ref, pot_ref, send, recv, extra, basis, inner, outb, outx, pots, mix,
           note, heard, send_sem, recv_sem, extra_send, extra_recv, pot_send, pot_recv, back_send, back_recv,
           far_send, note_send, note_recv, psi_sem, pot_sem, held):
    me = lax.axis_index("dom")
    mesh_ids = pl.DeviceIdType.MESH
    barrier = pltpu.get_barrier_semaphore()

    ratio = -0.5 * far_weight
    half = n // 2
    reach = ITERS - 1
    deep = half - reach
    side = me // half
    base = side * half
    opposite = half - base
    partner = lax.rem(me + half, n)
    near = half - side * reach
    outer = jnp.logical_or(me < deep, me >= n - deep)
    plane = n // 4
    spot = lax.rem(me, plane)
    inward = jnp.logical_and(me >= plane, me < n - plane)
    far_plane = (1 - side) * (n - plane)
    outward = jnp.logical_not(inward)

    def greet(k, carry):
        pl.semaphore_signal(barrier, inc=1, device_id={"dom": lax.rem(me + k, n)}, device_id_type=mesh_ids)
        return carry

    lax.fori_loop(1, n, greet, 0)

    def take_psi(x):
        part = pl.ds(x * (nx // 2), nx // 2)
        return pltpu.make_async_copy(psi_hbm.at[:, part], psi_ref.at[:, part], psi_sem.at[x])

    take_pot = pltpu.make_async_copy(pot_hbm, pot_ref, pot_sem)
    take_pot.start()
    for x in range(2):
        take_psi(x).start()

    def remote(src, dst, send_to, recv_to, there):
        return pltpu.make_async_remote_copy(
            src_ref=src, dst_ref=dst, send_sem=send_to, recv_sem=recv_to,
            device_id={"dom": there}, device_id_type=mesh_ids)

    def forward(c, here, there):
        return remote(send.at[c, there], recv.at[c, here + 1], send_sem, recv_sem.at[c, here // plane], there)

    def beside(c, here, there):
        return remote(send.at[c, lax.rem(there + half, n)], extra.at[c, lax.rem(here, half) + 1],
                      extra_send, extra_recv.at[c], there)

    def pot_copy(here, there):
        return remote(pots.at[me], pots.at[here], pot_send, pot_recv, there)

    def backward(c, owner, there):
        return remote(outb.at[c, there], back.at[c, owner], back_send, back_recv.at[c], there)

    def far_copy(c, i, there):
        return remote(outx.at[c, i], back.at[c, partner], far_send, back_recv.at[c], there)

    def note_copy(c):
        return remote(note.at[c], heard.at[c], note_send, note_recv.at[c], partner)

    def pack(x, carry):
        parts = [psi_ref[p, x].T.reshape(n, SUB, LANES) for p in range(2)]
        for c, block in enumerate(interleave(*parts, n)):
            send[c, :, x] = block
        return carry

    for x in range(2):
        take_psi(x).wait()
        lax.fori_loop(x * (nx // 2), (x + 1) * (nx // 2), pack, 0, unroll=True)

    take_pot.wait()
    pot_rows = jnp.concatenate([pot_ref[:, j, :] for j in range(LANES // nz)], axis=1)
    pots[me] = (pot_rows + -0.5 * centre_weight) * (1.0 / ratio)
    blank = jnp.zeros((nx, SUB, LANES), jnp.float32)
    for c in range(CHUNKS):
        recv[c, me + 1] = send[c, me]
        recv[c, 0] = blank
        recv[c, n + 1] = blank
        extra[c, me - base + 1] = send[c, partner]
        extra[c, 0] = blank
        extra[c, half + 1] = blank
    for j in range(ITERS - 1):
        basis[j, 0] = blank
        basis[j, n + 1] = blank
        inner[j, 0] = blank
        inner[j, half + 1] = blank

    pl.semaphore_wait(barrier, n - 1)

    def send_pot(k, carry):
        pot_copy(me, lax.rem(me + k, n)).start()
        return carry

    lax.fori_loop(1, n, send_pot, 0)

    def send_far(c):
        def one(k, carry):
            forward(c, me, far_plane + lax.rem(spot + k, plane)).start()
            return carry

        lax.fori_loop(0, plane, one, 0)

    def send_near(c):
        def one(k, carry):
            forward(c, me, plane * (2 - side) + lax.rem(spot + k, plane)).start()
            return carry

        lax.fori_loop(0, plane, one, 0)

    def send_plane(c):
        def one(k, carry):
            forward(c, me, me - spot + lax.rem(spot + k, plane)).start()
            return carry

        lax.fori_loop(1, plane, one, 0)

    def send_next(c):
        def one(k, carry):
            forward(c, me, base + lax.rem(me - spot - base + plane, half) + lax.rem(spot + k, plane)).start()
            return carry

        lax.fori_loop(0, plane, one, 0)

    def send_beside(c):
        def one(k, carry):
            beside(c, me, base + lax.rem(me + k, half)).start()
            return carry

        lax.fori_loop(1, half, one, 0)

    def landed(blocks, arrived):
        remote(blocks, blocks, note_send, arrived, partner).wait_recv()

    def left(blocks, departed):
        remote(blocks, blocks, departed, note_recv.at[0], partner).wait_send()

    upper = lax.broadcasted_iota(jnp.int32, (SUB, LANES), 1) >= nz
    lane = lax.broadcasted_iota(jnp.int32, (SUB, LANES), 1)
    sign = jnp.where(lax.broadcasted_iota(jnp.int32, (SUB, LANES), 0) < HALF, 1.0, -1.0)

    row = lax.broadcasted_iota(jnp.int32, (LANES, LANES), 0)
    column = lax.broadcasted_iota(jnp.int32, (LANES, LANES), 1)
    apart = lax.rem(row - column + 2 * nz, nz)
    near_z = jnp.where(jnp.logical_or(apart == 1, apart == nz - 1), 16.0, 0.0)
    far_z = jnp.where(jnp.logical_or(apart == 2, apart == nz - 2), 1.0, 0.0)
    same = (row < nz) == (column < nz)
    lanes_matrix = jnp.where(same, far_z - near_z, jnp.where(apart == 0, -16.0, 0.0)).astype(jnp.bfloat16)
    mix[0:LANES] = lanes_matrix
    mix[LANES:2 * LANES] = lanes_matrix

    def applied_at(ref, s, slab, size):
        slabs = [[ref[s + g, x] for x in range(nx)] for g in range(size + 2)]
        inside = jnp.concatenate([u for row_of in slabs[1:-1] for u in row_of], axis=0)
        high = inside.astype(jnp.bfloat16)
        rest = (inside - high.astype(jnp.float32)).astype(jnp.bfloat16)
        mixed = jnp.dot(jnp.concatenate([high, rest], axis=1), mix[...], preferred_element_type=jnp.float32)
        result = []
        for g in range(size):
            before, now, after = slabs[g:g + 3]
            for x in range(nx):
                u = now[x]
                close = now[(x + 1) % nx] + now[(x - 1) % nx]
                close = close + pltpu.roll(jnp.where(upper, before[x], after[x]), nz, 1)
                wide = now[(x + 2) % nx] + now[(x - 2) % nx] + before[x] + after[x]
                at = (g * nx + x) * SUB
                wide = wide + mixed[at:at + SUB]
                own = jnp.broadcast_to(pots[slab + g, pl.ds(x, 1), :], (SUB, LANES))
                result.append((own * u + (wide - 16.0 * close), u))
        return result

    def blend(us, straight, crossed):
        a = straight[0] * us[0]
        b = crossed[0] * us[0]
        for j in range(1, ITERS):
            a = a + straight[j] * us[j]
            b = b + crossed[j] * us[j]
        return a + swap_parts(b)

    @pl.when(outward)
    def _():
        send_next(0)
        send_plane(0)
        send_far(0)
        send_near(0)
        send_next(1)
        send_plane(1)
        send_far(1)
        send_near(1)
        send_beside(0)
        send_beside(1)

    @pl.when(inward)
    def _():
        send_plane(0)
        send_near(0)
        send_far(0)
        send_next(0)
        send_next(1)
        send_plane(1)
        send_beside(0)
        send_beside(1)
        landed(recv.at[0, pl.ds(0, plane)], recv_sem.at[0, far_plane // plane])
        send_near(1)
        send_far(1)

    def chunk(c, carry):
        vectors = [recv.at[c]] + [basis.at[j] for j in range(ITERS - 1)]

        own = me // plane * plane
        beyond = base + lax.rem(me - base + plane, half) // plane * plane
        across = plane * (2 - side)
        acc = jnp.zeros((SUB, LANES), jnp.float32)
        for first, count in ((own, plane - 1), (beyond, plane), (across, plane), (far_plane, plane)):
            blocks = recv.at[c, pl.ds(0, count)]
            arrived = recv_sem.at[c, first // plane]
            if first is far_plane:
                @pl.when(jnp.logical_not(jnp.logical_and(inward, c == 0)))
                def _(blocks=blocks, arrived=arrived):
                    landed(blocks, arrived)
            else:
                landed(blocks, arrived)

            def sum_up(k, acc, first=first):
                for x in range(nx):
                    u = recv[c, first + k + 1, x]
                    acc = acc + u * u
                return acc

            acc = lax.fori_loop(0, plane, sum_up, acc, unroll=True)
        square = total_of(acc) + epsilon
        scale = lax.rsqrt(square)
        first_norm = square * scale

        @pl.when(c == 0)
        def _():
            landed(pots.at[pl.ds(0, n - 1)], pot_recv)

        scales, steps = [scale], []
        alphas, betas, selves, previous = [], [], [], []
        zero = jnp.zeros((SUB, LANES), jnp.float32)
        for j in range(ITERS):
            ref = vectors[j]
            products = [zero, zero]
            squares = [zero, zero]
            done = 0
            for g in range(n // GROUP + 1):
                if j and g < n // GROUP:
                    for s in range(g * GROUP, (g + 1) * GROUP):
                        for x in range(nx):
                            r = steps[-1] * held[(j - 1) % 2, s, x] - selves[-1] * vectors[j - 1][s + 1, x]
                            if j > 1:
                                r = r - previous[-1] * vectors[j - 2][s + 1, x]
                            ref[s + 1, x] = r
                            squares[x % 2] = squares[x % 2] + r * r
                if j and g == n // GROUP:
                    square = total_of(squares[0] + squares[1]) + epsilon
                upto = n if g == n // GROUP else (g + 1) * GROUP - 1
                for at, (w, u) in enumerate(applied_at(ref, done, done, upto - done)):
                    if j + 1 < ITERS:
                        held[j % 2, done + at // nx, at % nx] = w
                    products[at % 2] = products[at % 2] + u * w
                done = upto
            if j:
                scale = lax.rsqrt(square)
                scales.append(scale)
                betas.append(square * scale)
            step = scale * ratio
            alpha = step * (scale * total_of(products[0] + products[1]))
            alphas.append(alpha)
            if j + 1 < ITERS:
                steps.append(step)
                selves.append(alpha * scale)
                previous.append(betas[-1] * scales[-2] if j else None)

        real, imag = krylov_weights(alphas, betas)
        straight = [first_norm * scales[j] * real[j] for j in range(ITERS)]
        crossed = [first_norm * scales[j] * imag[j] * sign for j in range(ITERS)]

        told = zero
        for k, value in enumerate(steps + selves + previous[1:] + straight + crossed):
            told = jnp.where(lane == k, value, told)
        note[c] = told

        def combined(d, x):
            return blend([v[d + 1, x] for v in vectors], straight, crossed)

        def finish_across(k, carry):
            there = near + lax.rem(me + k, reach)
            for x in range(nx):
                outb[c, there, x] = combined(there, x)

            @pl.when(k == 0)
            def _():
                note_copy(c).start()

            @pl.when(jnp.logical_and(k == 1, jnp.logical_and(c > 0, inward)))
            def _():
                def late(i, carry):
                    backward(c - 1, me, near + lax.rem(me + i, reach)).start()
                    return carry

                lax.fori_loop(0, reach, late, 0)

            @pl.when(jnp.logical_and(k > 0, jnp.logical_or(c == CHUNKS - 1, jnp.logical_not(inward))))
            def _():
                backward(c, me, near + lax.rem(me + k - 1, reach)).start()

            return carry

        lax.fori_loop(0, reach, finish_across, 0)

        def finish_home(k, carry):
            there = base + lax.rem(me + k, half)
            for x in range(nx):
                outb[c, there, x] = combined(there, x)

            @pl.when(jnp.logical_and(k == 1, jnp.logical_or(c == CHUNKS - 1, jnp.logical_not(inward))))
            def _():
                backward(c, me, near + lax.rem(me + reach - 1, reach)).start()

            @pl.when(k > 1)
            def _():
                backward(c, me, base + lax.rem(me + k - 1, half)).start()

            return carry

        lax.fori_loop(1, half, finish_home, 0)
        for x in range(nx):
            back[c, me, x] = combined(me, x)
        backward(c, me, base + lax.rem(me + half - 1, half)).start()

        return carry

    def assist(c, carry):
        landed(extra.at[c, pl.ds(0, half - 1)], extra_recv.at[c])
        note_copy(c).wait_recv()
        words = heard[c]
        word = [jnp.broadcast_to(words[:, k:k + 1], (SUB, LANES)) for k in range(3 * reach - 1 + 2 * ITERS)]
        steps, selves, previous = word[:reach], word[reach:2 * reach], [None] + word[2 * reach:3 * reach - 1]
        straight, crossed = word[3 * reach - 1:3 * reach - 1 + ITERS], word[3 * reach - 1 + ITERS:]

        halves = [extra.at[c]] + [inner.at[j] for j in range(reach)]
        for j in range(reach):
            count = half - 1 - j
            start = (j + 1) * side
            pieces = -(-count // GROUP)
            at = 0
            for piece in range(pieces):
                size = (count - at) // (pieces - piece)
                for i, (w, u) in enumerate(applied_at(halves[j], start + at, base + start + at, size)):
                    here = start + at + i // nx + 1
                    r = steps[j] * w - selves[j] * u
                    if j:
                        r = r - previous[j] * halves[j - 1][here, i % nx]
                    halves[j + 1][here, i % nx] = r
                at += size

        first = reach * side
        for i in range(deep):
            for x in range(nx):
                outx[c, i, x] = blend([v[first + i + 1, x] for v in halves], straight, crossed)
        for i in range(deep):
            there = base + first + i

            @pl.when(there == me)
            def _(i=i):
                back[c, partner] = outx[c, i]

            @pl.when(there != me)
            def _(i=i, there=there):
                far_copy(c, i, there).start()

        return carry

    lax.fori_loop(0, CHUNKS, chunk, 0)
    lax.fori_loop(0, CHUNKS, assist, 0)

    left(pots.at[pl.ds(0, n - 1)], pot_send)
    left(send.at[:, pl.ds(0, n - 1)], send_sem)
    left(send.at[:, pl.ds(0, half - 1)], extra_send)
    left(note, note_send)

    for mine, count in ((outer, n - 2), (jnp.logical_not(outer), n - 1)):
        @pl.when(mine)
        def _(count=count):
            for c in range(CHUNKS):
                landed(back.at[c, pl.ds(0, count)], back_recv.at[c])
            left(outx.at[:, pl.ds(0, count - n + 1 + deep)], far_send)

    left(outb.at[:, pl.ds(0, reach + half - 1)], back_send)


def fused(psi, potential, n):
    parts, slabs, nx, by, nz, orbs = psi.shape
    half, reach = n // 2, ITERS - 1
    vec = lambda *lead: pltpu.VMEM(lead + (nx, SUB, LANES), jnp.float32)
    tile = lambda *lead: pltpu.VMEM(lead + (SUB, LANES), jnp.float32)
    dma = lambda *shape: pltpu.SemaphoreType.DMA(shape)
    result = pl.pallas_call(
        functools.partial(kernel, n, nx, nz),
        out_shape=pltpu.VMEM((CHUNKS, n, nx, SUB, LANES), jnp.float32),
        in_specs=[pl.BlockSpec(memory_space=pl.ANY)] * 2,
        out_specs=pl.BlockSpec(memory_space=pltpu.VMEM),
        scratch_shapes=[
            pltpu.VMEM((parts, nx, by * nz, orbs), jnp.float32), pltpu.VMEM((nx, by, nz), jnp.float32),
            vec(CHUNKS, n), vec(CHUNKS, n + 2), vec(CHUNKS, half + 2), vec(reach, n + 2), vec(reach, half + 2),
            vec(CHUNKS, n), vec(CHUNKS, half - reach),
            pltpu.VMEM((n, nx, LANES), jnp.float32), pltpu.VMEM((2 * LANES, LANES), jnp.bfloat16),
            tile(CHUNKS), tile(CHUNKS),
            dma(), dma(CHUNKS, 4), dma(), dma(CHUNKS), dma(), dma(),
            dma(), dma(CHUNKS), dma(), dma(), dma(CHUNKS), dma(2), dma(), vec(2, n),
        ],
        compiler_params=pltpu.CompilerParams(collective_id=0, has_side_effects=True),
    )(psi.reshape(parts, nx, by * nz, orbs), potential.reshape(nx, by, nz))
    out = pl.pallas_call(
        functools.partial(unpack_kernel, n, nx),
        out_shape=jax.ShapeDtypeStruct((parts, nx, by * nz, orbs), jnp.float32),
        in_specs=[pl.BlockSpec(memory_space=pltpu.VMEM)],
        out_specs=pl.BlockSpec(memory_space=pl.ANY),
        scratch_shapes=[pltpu.VMEM((parts, nx, by * nz, orbs), jnp.float32), dma()],
    )(pltpu.with_memory_space_constraint(result, pltpu.VMEM))
    return out.reshape(psi.shape)


def fits(psi, n):
    parts, slabs, nx, by, nz, orbs = psi.shape
    return parts == 2 and slabs == 1 and by == 2 and by * nz == LANES and orbs == LANES and orbs == n * SUB and nx % 2 == 0 and n % GROUP == 0 and n // 2 > ITERS


def per_device(n, psi, potential):
    if fits(psi, n):
        return fused(psi, potential, n)
    return on_device(psi, potential)


def solution(mesh):
    placed = (P(None, "dom", None, None, None, "st"), P("dom", None, None, None))
    return jax.shard_map(
        functools.partial(per_device, mesh.shape["dom"]),
        mesh=mesh,
        in_specs=placed,
        out_specs=P(None, "dom", None, None, None, "st"),
        check_vma=False,
    )
```
